32 devices in a mesh: row: 4 (over y, x), col: 8 (over z, core).
Axes of the slice: x: 2, y: 2, z: 4, core: 2. Of those that a mesh axis runs over, the one named last changes fastest.
Arguments:
- e_field: float32 [3, 64, 32, 1024], P(None, None, 'row', 'col'), may hold values from -6 to 6
- h_field: float32 [3, 64, 32, 1024], P(None, None, 'row', 'col'), may hold values from -6 to 6
- e_coef: float32 [64, 32, 1024], P(None, 'row', 'col'), may hold values from 0.125 to 0.5
- basis: float32 [128, 32, 1024], P('row', None, 'col'), may hold values from -0.03125 to 0.03125
- pml_width: int32 [4], replicated, may hold values from 2 to 8
- snap_index: int32 [64], replicated, may hold values from 0 to 383
Outputs:
- e_final: float32 [3, 64, 32, 1024], P(None, None, 'row', 'col')
- h_final: float32 [3, 64, 32, 1024], P(None, None, 'row', 'col')
- coefficients: float32 [64, 128], replicated
- gram: float32 [64, 64], replicated
The draws below stay inside these ranges and needn't reach their ends.
All inputs are finite; a program needn't handle non-finite values.
Results may differ from the reference program's by a relative error of at most 0.00008.
Values sent between devices are 32-bit elements; how exact they have to be, the bound alone decides.
A program may use at most 64 MiB of HBM per device.

```python
import math
import jax
import jax.numpy as jnp
from jax import lax

NZ = 64
STEPS = 8
RANK = 128
SNAPS = 64
NX = 32
NY = 1024


def place_ends(entries, own_key, low, high):
    spot = [jax.random.randint(jax.random.fold_in(own_key, axis), (), 0, length) for axis, length in enumerate(entries.shape)]
    main_axis = entries.shape.index(max(entries.shape))
    next_to = spot[:main_axis] + [(spot[main_axis] + 1) % entries.shape[main_axis]] + spot[main_axis + 1:]
    return entries.at[tuple(spot)].set(low).at[tuple(next_to)].set(high)


def level_of(rng, shape, shards, smallest, top_value):
    level, own = 1.0, jax.random.fold_in(rng, 6)
    for position, blocks in shards:
        draws = jnp.exp(jax.random.uniform(jax.random.fold_in(own, position), (blocks,), jnp.float32, smallest / len(shards), top_value / len(shards)))
        level = level * jnp.repeat(draws, shape[position] // blocks).reshape([-1 if axis == position else 1 for axis in range(len(shape))])
    return level


def normal_values(own_key, dims, width, limit, cuts=(), held_as=jnp.bfloat16):
    result = jax.random.normal(own_key, dims, jnp.float32) * width
    if len(cuts) > 0:
        result = level_of(own_key, dims, cuts, -0.22, 0.18) * result
    return jnp.clip(result, min=-limit, max=limit).astype(held_as)


def setup_inputs(seed: int = 0) -> dict:
    key_list = jax.random.split(jax.random.key(seed), 7)
    e_field = normal_values(key_list[0], (3, NZ, NX, NY), 1.0, 6.0, ((2, 4), (3, 8)), jnp.float32)
    h_field = normal_values(key_list[1], (3, NZ, NX, NY), 1.0, 6.0, ((2, 4), (3, 8)), jnp.float32)
    e_coef = jnp.clip(jnp.exp(math.log(0.5) - 1.3862944 * jax.random.uniform(key_list[2], (NZ, NX, NY), jnp.float32) ** level_of(key_list[2], (NZ, NX, NY), ((1, 4), (2, 8)), -0.2, 0.2)), 0.125, 0.5)
    basis = normal_values(key_list[3], (RANK, NX, NY), (NX * NY) ** -0.5, 0.03125, ((0, 4), (2, 8)), jnp.float32)
    pml_width = place_ends(jax.random.randint(key_list[4], (4,), 2, 9), jax.random.fold_in(key_list[4], 1), 2, 8).astype(jnp.int32)
    snap_index = place_ends(jax.random.randint(key_list[5], (SNAPS,), 0, 6 * NZ), jax.random.fold_in(key_list[5], 1), 0, (6 * NZ) - 1).astype(jnp.int32)
    return {"e_field": e_field, "h_field": h_field, "e_coef": e_coef, "basis": basis, "pml_width": pml_width, "snap_index": snap_index}


time_step = 0.5
sigma_top = 4.0
alpha_shift = 0.05


def forward(field, axis, plane):
    count = field.shape[axis]
    after = jnp.concatenate([lax.slice_in_dim(field, 1, count, axis=axis), jnp.expand_dims(plane, axis)], axis)
    return after - field


def backward(field, axis, plane):
    count = field.shape[axis]
    before = jnp.concatenate([jnp.expand_dims(plane, axis), lax.slice_in_dim(field, 0, count - 1, axis=axis)], axis)
    return field - before


def absorber(positions, total, low, high):
    depth = jnp.maximum(jnp.maximum((low - positions) / low, (positions - (total - 1.0 - high)) / high), 0.0)
    sigma = sigma_top * depth ** 3
    damp = jnp.exp(-(sigma + alpha_shift) * time_step)
    gain = sigma / (sigma + alpha_shift) * (damp - 1.0)
    return damp, gain


def magnetic(e_field, h_field, psi, next_x, next_y, damp_x, gain_x, damp_y, gain_y):
    e_x, e_y, e_z = e_field[0], e_field[1], e_field[2]
    h_x, h_y, h_z = h_field[0], h_field[1], h_field[2]
    zplane = jnp.zeros_like(e_x[0])
    ez_dy = forward(e_z, 2, next_y[1])
    ey_dz = forward(e_y, 0, zplane)
    ex_dz = forward(e_x, 0, zplane)
    ez_dx = forward(e_z, 1, next_x[1])
    ey_dx = forward(e_y, 1, next_x[0])
    ex_dy = forward(e_x, 2, next_y[0])
    psi_hxy = damp_y * psi[0] + gain_y * ez_dy
    psi_hyx = damp_x * psi[1] + gain_x * ez_dx
    psi_hzx = damp_x * psi[2] + gain_x * ey_dx
    psi_hzy = damp_y * psi[3] + gain_y * ex_dy
    h_x = h_x - time_step * (ez_dy + psi_hxy - ey_dz)
    h_y = h_y - time_step * (ex_dz - ez_dx - psi_hyx)
    h_z = h_z - time_step * (ey_dx + psi_hzx - ex_dy - psi_hzy)
    return jnp.stack((h_x, h_y, h_z)), (psi_hxy, psi_hyx, psi_hzx, psi_hzy)


def electric(e_field, h_field, psi, e_coef, prev_x, prev_y, damp_x, gain_x, damp_y, gain_y):
    e_x, e_y, e_z = e_field[0], e_field[1], e_field[2]
    h_x, h_y, h_z = h_field[0], h_field[1], h_field[2]
    zplane = jnp.zeros_like(h_x[0])
    hz_dy = backward(h_z, 2, prev_y[1])
    hy_dz = backward(h_y, 0, zplane)
    hx_dz = backward(h_x, 0, zplane)
    hz_dx = backward(h_z, 1, prev_x[1])
    hy_dx = backward(h_y, 1, prev_x[0])
    hx_dy = backward(h_x, 2, prev_y[0])
    psi_exy = damp_y * psi[0] + gain_y * hz_dy
    psi_eyx = damp_x * psi[1] + gain_x * hz_dx
    psi_ezx = damp_x * psi[2] + gain_x * hy_dx
    psi_ezy = damp_y * psi[3] + gain_y * hx_dy
    e_x = e_x + e_coef * (hz_dy + psi_exy - hy_dz)
    e_y = e_y + e_coef * (hx_dz - hz_dx - psi_eyx)
    e_z = e_z + e_coef * (hy_dx + psi_ezx - hx_dy - psi_ezy)
    return jnp.stack((e_x, e_y, e_z)), (psi_exy, psi_eyx, psi_ezx, psi_ezy)


def reference(e_field, h_field, e_coef, basis, pml_width, snap_index):
    widths = pml_width.astype(jnp.float32)
    x_pos = jnp.arange(NX, dtype=jnp.float32)
    y_pos = jnp.arange(NY, dtype=jnp.float32)
    hdx, hgx = absorber(x_pos + 0.5, float(NX), widths[0], widths[1])
    hdy, hgy = absorber(y_pos + 0.5, float(NY), widths[2], widths[3])
    edx, egx = absorber(x_pos, float(NX), widths[0], widths[1])
    edy, egy = absorber(y_pos, float(NY), widths[2], widths[3])
    hdx, hgx, edx, egx = [v.reshape(1, NX, 1) for v in (hdx, hgx, edx, egx)]
    hdy, hgy, edy, egy = [v.reshape(1, 1, NY) for v in (hdy, hgy, edy, egy)]
    zeros_cells = jnp.zeros((NZ, NX, NY), jnp.float32)
    psi_mag = (zeros_cells,) * 4
    psi_ele = (zeros_cells,) * 4
    plane_x = jnp.zeros((2, NZ, NY), jnp.float32)
    plane_y = jnp.zeros((2, NZ, NX), jnp.float32)
    for step in range(STEPS):
        h_field, psi_mag = magnetic(e_field, h_field, psi_mag, plane_x, plane_y, hdx, hgx, hdy, hgy)
        e_field, psi_ele = electric(e_field, h_field, psi_ele, e_coef, plane_x, plane_y, edx, egx, edy, egy)
    planes = jnp.concatenate((e_field, h_field), 0).reshape(6 * NZ, NX, NY)
    snaps = jnp.take(planes, snap_index, axis=0).reshape(SNAPS, NX * NY)
    coefficients = jnp.dot(snaps, basis.reshape(RANK, NX * NY).T, precision=lax.Precision.HIGHEST)
    gram = jnp.dot(snaps, snaps.T, precision=lax.Precision.HIGHEST) / float(NX * NY)
    return e_field, h_field, coefficients, gram
```

```python
import functools
import jax
import jax.numpy as jnp
from jax import lax
from jax.experimental import pallas as pl
from jax.experimental.pallas import tpu as pltpu
from jax.sharding import PartitionSpec as P

STEPS = 8
UNROLL = 4

time_step = 0.5
sigma_top = 4.0
alpha_shift = 0.05


def absorber(positions, total, low, high):
    depth = jnp.maximum(
        jnp.maximum((low - positions) / low, (positions - (total - 1.0 - high)) / high), 0.0
    )
    sigma = sigma_top * (depth * depth * depth)
    damp = jnp.exp(-(sigma + alpha_shift) * time_step)
    gain = sigma / (sigma + alpha_shift) * (damp - 1.0)
    return damp, gain


def step_kernel(
    n_row, n_col, width_ref, e_in, h_in, coef_in, e_out, h_out,
    e_s, h_s, coef_s, psi, first_x, last_x, h_last_x, first_y, last_y, h_last_y,
    next_x, prev_x, halo_x, halo_psi_x, next_y, prev_y, corner_x, corner_y, halo_y, halo_psi_y,
    prof, local_sem, send_sem, recv_sem, once_send, once_recv,
):
    nz, nx, ny = coef_s.shape
    row, col = lax.axis_index("row"), lax.axis_index("col")
    up, down = row > 0, row < n_row - 1
    left, right = col > 0, col < n_col - 1
    sw = jnp.logical_and(down, left)
    ne = jnp.logical_and(up, right)
    routes = (
        (up, {"row": row - 1, "col": col}), (down, {"row": row + 1, "col": col}),
        (left, {"row": row, "col": col - 1}), (sw, {"row": row + 1, "col": col - 1}),
        (right, {"row": row, "col": col + 1}), (ne, {"row": row - 1, "col": col + 1}),
    )

    load_e = pltpu.make_async_copy(e_in, e_s.at[:, pl.ds(0, nz)], local_sem.at[0])
    load_h = pltpu.make_async_copy(h_in, h_s.at[:, pl.ds(1, nz)], local_sem.at[1])
    load_c = pltpu.make_async_copy(coef_in, coef_s, local_sem.at[2])
    load_e.start()
    load_h.start()
    load_c.start()

    next_x[...] = jnp.zeros_like(next_x)
    prev_x[...] = jnp.zeros_like(prev_x)
    halo_x[...] = jnp.zeros_like(halo_x)
    halo_psi_x[...] = jnp.zeros_like(halo_psi_x)
    next_y[...] = jnp.zeros_like(next_y)
    prev_y[...] = jnp.zeros_like(prev_y)
    corner_x[...] = jnp.zeros_like(corner_x)
    corner_y[...] = jnp.zeros_like(corner_y)
    halo_y[...] = jnp.zeros_like(halo_y)
    halo_psi_y[...] = jnp.zeros_like(halo_psi_y)

    barrier = pltpu.get_barrier_semaphore()
    for there, where in routes:
        @pl.when(there)
        def _():
            pl.semaphore_signal(barrier, inc=1, device_id=where, device_id_type=pl.DeviceIdType.MESH)

    zero = jnp.zeros((nx, ny), jnp.float32)
    for c in range(3):
        e_s[c, nz] = zero
        h_s[c, 0] = zero

    def clear(z, carry):
        for k in range(8):
            psi[k, z] = zero
        return carry

    lax.fori_loop(0, nz, clear, 0)

    sub = lax.broadcasted_iota(jnp.int32, (nx, ny), 0)
    lane = lax.broadcasted_iota(jnp.int32, (nx, ny), 1)
    w = [jnp.full((nx, ny), width_ref[k], jnp.int32).astype(jnp.float32) for k in range(4)]
    x_pos = (sub + row * nx).astype(jnp.float32)
    y_pos = (lane + col * ny).astype(jnp.float32)
    x_before = (jnp.zeros_like(sub) + (row * nx - 1)).astype(jnp.float32)
    y_before = (jnp.zeros_like(sub) + (col * ny - 1)).astype(jnp.float32)
    full_x, full_y = float(nx * n_row), float(ny * n_col)
    pairs = (
        absorber(x_pos + 0.5, full_x, w[0], w[1]), absorber(y_pos + 0.5, full_y, w[2], w[3]),
        absorber(x_pos, full_x, w[0], w[1]), absorber(y_pos, full_y, w[2], w[3]),
        absorber(x_before + 0.5, full_x, w[0], w[1]), absorber(y_before + 0.5, full_y, w[2], w[3]),
    )
    for k, (damp, gain) in enumerate(pairs):
        prof[2 * k] = damp
        prof[2 * k + 1] = gain

    def pack(z, ex, ey, ez, cols):
        first, last0, last1 = cols
        first_x[0, pl.ds(z, 1), :] = ey[0:1]
        first_x[1, pl.ds(z, 1), :] = ez[0:1]
        last_x[0, pl.ds(z, 1), :] = ex[nx - 1:nx]
        last_x[1, pl.ds(z, 1), :] = ey[nx - 1:nx]
        last_x[2, pl.ds(z, 1), :] = ez[nx - 1:nx]
        rx = pltpu.roll(ex, z, 1)
        rz = pltpu.roll(ez, z + nz, 1)
        ry = pltpu.roll(ey, z, 1)
        first = jnp.where(lane == z, rx, jnp.where(lane == z + nz, rz, first))
        before = lax.rem(z + ny - 1, ny)
        last0 = jnp.where(lane == before, rx, jnp.where(lane == z + nz - 1, rz, last0))
        last1 = jnp.where(lane == before, ry, last1)
        return first, last0, last1

    def keep(cols):
        first_y[...] = cols[0]
        last_y[0] = pltpu.roll(cols[1], 1, 1)
        last_y[1] = pltpu.roll(cols[2], 1, 1)

    def copies(slot):
        parts = (
            (first_x, next_x.at[slot]),
            (last_x, prev_x.at[slot, :, pl.ds(0, nz)]),
            (first_y, next_y.at[slot]),
            (first_y, corner_x.at[slot]),
            (last_y, prev_y.at[slot]),
            (last_y.at[1], corner_y.at[slot]),
        )
        return [
            pltpu.make_async_remote_copy(
                src_ref=src, dst_ref=dst, send_sem=send_sem.at[m, slot], recv_sem=recv_sem.at[m, slot],
                device_id=routes[m][1], device_id_type=pl.DeviceIdType.MESH)
            for m, (src, dst) in enumerate(parts)
        ]

    def start_all(slot):
        for m, copy in enumerate(copies(slot)):
            @pl.when(routes[m][0])
            def _():
                copy.start()

    arrives = (down, up, right, ne, left, sw)

    def wait_recv(slot, which):
        every = copies(slot)
        for m in which:
            @pl.when(arrives[m])
            def _():
                every[m].wait_recv()

    def wait_send(slot):
        for m, copy in enumerate(copies(slot)):
            @pl.when(routes[m][0])
            def _():
                copy.wait_send()

    load_e.wait()
    load_h.wait()

    def first_pack(k, carry):
        cols, hcol = carry
        for j in range(UNROLL):
            z = k * UNROLL + j
            cols = pack(z, e_s[0, z], e_s[1, z], e_s[2, z], cols)
            hx, hy, hz = h_s[0, z + 1], h_s[1, z + 1], h_s[2, z + 1]
            h_last_x[0, pl.ds(z, 1), :] = hy[nx - 1:nx]
            h_last_x[1, pl.ds(z, 1), :] = hz[nx - 1:nx]
            hcol = jnp.where(lane == z, pltpu.roll(hz, z + 1, 1), hcol)
            hcol = jnp.where(lane == z + nz, pltpu.roll(hx, lax.rem(z + nz + 1, ny), 1), hcol)
        return cols, hcol

    cols, hcol = lax.fori_loop(0, nz // UNROLL, first_pack, ((zero, zero, zero), zero))
    keep(cols)
    h_last_y[...] = hcol

    count = sum(there.astype(jnp.int32) for there, _ in routes)
    pl.semaphore_wait(barrier, count)
    once = [
        pltpu.make_async_remote_copy(
            src_ref=src, dst_ref=dst, send_sem=once_send.at[k], recv_sem=once_recv.at[k],
            device_id=routes[m][1], device_id_type=pl.DeviceIdType.MESH)
        for k, (src, dst, m) in enumerate(((h_last_x, halo_x, 1), (h_last_y, halo_y, 4)))
    ]
    start_all(0)
    for k, m in enumerate((1, 4)):
        @pl.when(routes[m][0])
        def _():
            once[k].start()
    load_c.wait()

    def magnetic(slot):
        hdx, hgx, hdy, hgy = prof[0], prof[1], prof[2], prof[3]
        edge = next_y[slot]

        def body(k, carry):
            for j in range(UNROLL):
                z = k * UNROLL + j
                ex, ey, ez = e_s[0, z], e_s[1, z], e_s[2, z]
                row_y = jnp.broadcast_to(next_x[slot, 0, pl.ds(z, 1), :], (nx, ny))
                row_z = jnp.broadcast_to(next_x[slot, 1, pl.ds(z, 1), :], (nx, ny))
                col_x = pltpu.roll(edge, ny - 1 - z, 1)
                col_z = pltpu.roll(edge, ny - 1 - nz - z, 1)
                ey_dz = e_s[1, z + 1] - ey
                ex_dz = e_s[0, z + 1] - ex
                ez_dy = jnp.where(lane == ny - 1, col_z, pltpu.roll(ez, ny - 1, 1)) - ez
                ex_dy = jnp.where(lane == ny - 1, col_x, pltpu.roll(ex, ny - 1, 1)) - ex
                ez_dx = jnp.where(sub == nx - 1, row_z, pltpu.roll(ez, nx - 1, 0)) - ez
                ey_dx = jnp.where(sub == nx - 1, row_y, pltpu.roll(ey, nx - 1, 0)) - ey
                p0 = hdy * psi[0, z] + hgy * ez_dy
                p1 = hdx * psi[1, z] + hgx * ez_dx
                p2 = hdx * psi[2, z] + hgx * ey_dx
                p3 = hdy * psi[3, z] + hgy * ex_dy
                psi[0, z], psi[1, z], psi[2, z], psi[3, z] = p0, p1, p2, p3
                h_s[0, z + 1] = h_s[0, z + 1] - time_step * (ez_dy + p0 - ey_dz)
                h_s[1, z + 1] = h_s[1, z + 1] - time_step * (ex_dz - ez_dx - p1)
                h_s[2, z + 1] = h_s[2, z + 1] - time_step * (ey_dx + p2 - ex_dy - p3)
            return carry

        lax.fori_loop(0, nz // UNROLL, body, 0)

    def magnetic_row_before(slot):
        hdy, hgy = prof[2][0:1], prof[3][0:1]
        hdx, hgx = prof[8][0:1], prof[9][0:1]
        ex, ey, ez = prev_x[slot, 0, 0:nz], prev_x[slot, 1, 0:nz], prev_x[slot, 2, 0:nz]
        big_lane = lax.broadcasted_iota(jnp.int32, (nz, ny), 1)
        big_z = lax.broadcasted_iota(jnp.int32, (nz, ny), 0)
        corner = jnp.broadcast_to(corner_x[slot, nx - 1:nx, :], (nz, ny))
        corner = jnp.sum(jnp.where(big_lane == big_z, corner, 0.0), axis=1, keepdims=True)
        ex_dz = prev_x[slot, 0, 1:nz + 1] - ex
        ex_dy = jnp.where(big_lane == ny - 1, corner, pltpu.roll(ex, ny - 1, 1)) - ex
        ey_dx = first_x[0] - ey
        ez_dx = first_x[1] - ez
        p1 = hdx * halo_psi_x[0] + hgx * ez_dx
        p2 = hdx * halo_psi_x[1] + hgx * ey_dx
        p3 = hdy * halo_psi_x[2] + hgy * ex_dy
        halo_psi_x[0], halo_psi_x[1], halo_psi_x[2] = p1, p2, p3
        mask = up.astype(jnp.float32)
        halo_x[0] = mask * (halo_x[0] - time_step * (ex_dz - ez_dx - p1))
        halo_x[1] = mask * (halo_x[1] - time_step * (ey_dx + p2 - ex_dy - p3))

    def magnetic_column_before(slot):
        hdx, hgx = prof[0], prof[1]
        hdy, hgy = prof[10], prof[11]
        ey = prev_y[slot, 1]
        dy = first_y[...] - prev_y[slot, 0]
        below = jnp.broadcast_to(corner_y[slot, 0:1, :], (nx, ny))
        ey_dx = jnp.where(sub == nx - 1, below, pltpu.roll(ey, nx - 1, 0)) - ey
        ey_dz = pltpu.roll(pltpu.roll(ey, ny - 1, 1) - ey, nz, 1)
        py = hdy * halo_psi_y[0] + hgy * dy
        px = hdx * halo_psi_y[1] + hgx * ey_dx
        halo_psi_y[0], halo_psi_y[1] = py, px
        mask = left.astype(jnp.float32)
        change = jnp.where(lane < nz, ey_dx + px - dy - py, dy + py - ey_dz)
        halo_y[...] = mask * (halo_y[...] - time_step * change)

    def electric():
        edx, egx, edy, egy = prof[4], prof[5], prof[6], prof[7]
        edge = halo_y[...]

        def body(k, cols):
            for j in range(UNROLL):
                z = k * UNROLL + j
                hx, hy, hz = h_s[0, z + 1], h_s[1, z + 1], h_s[2, z + 1]
                row_y = jnp.broadcast_to(halo_x[0, pl.ds(z, 1), :], (nx, ny))
                row_z = jnp.broadcast_to(halo_x[1, pl.ds(z, 1), :], (nx, ny))
                col_z = pltpu.roll(edge, lax.rem(ny - z, ny), 1)
                col_x = pltpu.roll(edge, ny - nz - z, 1)
                hy_dz = hy - h_s[1, z]
                hx_dz = hx - h_s[0, z]
                hz_dy = hz - jnp.where(lane == 0, col_z, pltpu.roll(hz, 1, 1))
                hx_dy = hx - jnp.where(lane == 0, col_x, pltpu.roll(hx, 1, 1))
                hz_dx = hz - jnp.where(sub == 0, row_z, pltpu.roll(hz, 1, 0))
                hy_dx = hy - jnp.where(sub == 0, row_y, pltpu.roll(hy, 1, 0))
                p0 = edy * psi[4, z] + egy * hz_dy
                p1 = edx * psi[5, z] + egx * hz_dx
                p2 = edx * psi[6, z] + egx * hy_dx
                p3 = edy * psi[7, z] + egy * hx_dy
                psi[4, z], psi[5, z], psi[6, z], psi[7, z] = p0, p1, p2, p3
                amount = coef_s[z]
                ex = e_s[0, z] + amount * (hz_dy + p0 - hy_dz)
                ey = e_s[1, z] + amount * (hx_dz - hz_dx - p1)
                ez = e_s[2, z] + amount * (hy_dx + p2 - hx_dy - p3)
                e_s[0, z], e_s[1, z], e_s[2, z] = ex, ey, ez
                cols = pack(z, ex, ey, ez, cols)
            return cols

        keep(lax.fori_loop(0, nz // UNROLL, body, (zero, zero, zero)))

    def step(s, carry):
        slot = lax.rem(s, 2)
        wait_recv(slot, (0, 2))
        magnetic(slot)
        wait_recv(slot, (1, 3))

        @pl.when(s == 0)
        def _():
            for k, there in enumerate((up, left)):
                @pl.when(there)
                def _():
                    once[k].wait_recv()

        magnetic_row_before(slot)
        wait_recv(slot, (4, 5))
        magnetic_column_before(slot)
        wait_send(slot)
        electric()

        @pl.when(s < STEPS - 1)
        def _():
            start_all(1 - slot)

        return carry

    lax.fori_loop(0, STEPS, step, 0)
    for k, m in enumerate((1, 4)):
        @pl.when(routes[m][0])
        def _():
            once[k].wait_send()
    store_e = pltpu.make_async_copy(e_s.at[:, pl.ds(0, nz)], e_out, local_sem.at[0])
    store_h = pltpu.make_async_copy(h_s.at[:, pl.ds(1, nz)], h_out, local_sem.at[1])
    store_e.start()
    store_h.start()
    store_e.wait()
    store_h.wait()


def run_steps(e_field, h_field, e_coef, pml_width):
    nz, nx, ny = e_coef.shape
    n_row, n_col = lax.axis_size("row"), lax.axis_size("col")
    f32 = jnp.float32
    any_space = pl.BlockSpec(memory_space=pl.ANY)
    return pl.pallas_call(
        functools.partial(step_kernel, n_row, n_col),
        out_shape=[jax.ShapeDtypeStruct(e_field.shape, f32)] * 2,
        in_specs=[pl.BlockSpec(memory_space=pltpu.SMEM), any_space, any_space, any_space],
        out_specs=[any_space, any_space],
        scratch_shapes=[
            pltpu.VMEM((3, nz + 1, nx, ny), f32), pltpu.VMEM((3, nz + 1, nx, ny), f32),
            pltpu.VMEM((nz, nx, ny), f32), pltpu.VMEM((8, nz, nx, ny), f32),
            pltpu.VMEM((2, nz, ny), f32), pltpu.VMEM((3, nz, ny), f32), pltpu.VMEM((2, nz, ny), f32),
            pltpu.VMEM((nx, ny), f32), pltpu.VMEM((2, nx, ny), f32), pltpu.VMEM((nx, ny), f32),
            pltpu.VMEM((2, 2, nz, ny), f32), pltpu.VMEM((2, 3, nz + 8, ny), f32),
            pltpu.VMEM((2, nz, ny), f32), pltpu.VMEM((3, nz, ny), f32),
            pltpu.VMEM((2, nx, ny), f32), pltpu.VMEM((2, 2, nx, ny), f32),
            pltpu.VMEM((2, nx, ny), f32), pltpu.VMEM((2, nx, ny), f32),
            pltpu.VMEM((nx, ny), f32), pltpu.VMEM((2, nx, ny), f32),
            pltpu.VMEM((12, nx, ny), f32),
            pltpu.SemaphoreType.DMA((3,)),
            pltpu.SemaphoreType.DMA((6, 2)), pltpu.SemaphoreType.DMA((6, 2)),
            pltpu.SemaphoreType.DMA((2,)), pltpu.SemaphoreType.DMA((2,)),
        ],
        compiler_params=pltpu.CompilerParams(
            collective_id=0, has_side_effects=True, vmem_limit_bytes=32 * 1024 * 1024
        ),
    )(pml_width, e_field, h_field, e_coef)


def shards(e_field, h_field, e_coef, basis, pml_width, snap_index):
    depth_z, rows_here, cols_here = e_coef.shape
    full_x = rows_here * lax.axis_size("row")
    full_y = cols_here * lax.axis_size("col")
    e_field, h_field = run_steps(e_field, h_field, e_coef, pml_width)
    planes = jnp.concatenate((e_field, h_field), 0).reshape(6 * depth_z, rows_here, cols_here)
    snaps = jnp.take(planes, snap_index, axis=0)
    count = snaps.shape[0]
    flat = snaps.reshape(count, rows_here * cols_here)
    gram_part = jnp.dot(flat, flat.T, precision=lax.Precision.HIGHEST) / float(full_x * full_y)
    local_modes = lax.all_to_all(basis, "row", split_axis=1, concat_axis=0, tiled=True)
    coef_part = jnp.dot(
        flat, local_modes.reshape(local_modes.shape[0], -1).T, precision=lax.Precision.HIGHEST
    )
    coefficients, gram = lax.psum((coef_part, gram_part), ("row", "col"))
    return (e_field, h_field, coefficients, gram)


def solution(mesh):
    in_specs = (
        P(None, None, "row", "col"),
        P(None, None, "row", "col"),
        P(None, "row", "col"),
        P("row", None, "col"),
        P(),
        P(),
    )
    out_specs = (P(None, None, "row", "col"), P(None, None, "row", "col"), P(), P())
    return jax.shard_map(shards, mesh=mesh, in_specs=in_specs, out_specs=out_specs, check_vma=False)
```

```python
import functools
import jax
import jax.numpy as jnp
from jax import lax
from jax.experimental import pallas as pl
from jax.experimental.pallas import tpu as pltpu
from jax.sharding import PartitionSpec as P

STEPS = 8
UNROLL = 16

time_step = 0.5
sigma_top = 4.0
alpha_shift = 0.05


def absorber(positions, total, low, high):
    depth = jnp.maximum(
        jnp.maximum((low - positions) / low, (positions - (total - 1.0 - high)) / high), 0.0
    )
    sigma = sigma_top * (depth * depth * depth)
    damp = jnp.exp(-(sigma + alpha_shift) * time_step)
    gain = sigma / (sigma + alpha_shift) * (damp - 1.0)
    return damp, gain


def step_kernel(
    n_row, n_col, width_ref, index_ref, e_in, h_in, coef_in, basis_in, e_out, h_out, proj_out, gram_out,
    fields, coef_s, psi, first_x, last_x, h_last_x, first_y, last_y, h_last_y,
    next_x, prev_x, halo_x, halo_psi_x, next_y, prev_y, corner_x, corner_y, halo_y, halo_psi_y,
    prof, modes, snaps, part, row_sums, col_sums, total,
    local_sem, send_sem, recv_sem, once_send, once_recv, mode_send, mode_recv,
    sum_send, sum_recv, col_send, col_recv, back_send, back_recv,
):
    e_s, h_s = fields.at[pl.ds(0, 3)], fields.at[pl.ds(3, 3)]
    nz, nx, ny = coef_s.shape
    row, col = lax.axis_index("row"), lax.axis_index("col")
    up, down = row > 0, row < n_row - 1
    left, right = col > 0, col < n_col - 1
    sw = jnp.logical_and(down, left)
    ne = jnp.logical_and(up, right)
    routes = (
        (up, {"row": row - 1, "col": col}), (down, {"row": row + 1, "col": col}),
        (left, {"row": row, "col": col - 1}), (sw, {"row": row + 1, "col": col - 1}),
        (right, {"row": row, "col": col + 1}), (ne, {"row": row - 1, "col": col + 1}),
    )

    load_e = pltpu.make_async_copy(e_in, e_s.at[:, pl.ds(0, nz)], local_sem.at[0])
    load_h = pltpu.make_async_copy(h_in, h_s.at[:, pl.ds(1, nz)], local_sem.at[1])
    load_c = pltpu.make_async_copy(coef_in, coef_s, local_sem.at[2])
    load_e.start()
    load_h.start()
    load_c.start()
    n_modes = basis_in.shape[0]
    modes_3d = modes.reshape(n_modes * n_row, nx, ny)
    load_b = pltpu.make_async_copy(
        basis_in.at[:, pl.ds(pl.multiple_of(row * nx, nx), nx)],
        modes_3d.at[pl.ds(row * n_modes, n_modes)], local_sem.at[3])
    load_b.start()
    row_peers = [lax.rem(row + k, n_row) for k in range(1, n_row)]
    col_peers = [lax.rem(col + k, n_col) for k in range(1, n_col)]

    part[...] = jnp.zeros_like(part)
    next_x[...] = jnp.zeros_like(next_x)
    prev_x[...] = jnp.zeros_like(prev_x)
    halo_x[...] = jnp.zeros_like(halo_x)
    halo_psi_x[...] = jnp.zeros_like(halo_psi_x)
    next_y[...] = jnp.zeros_like(next_y)
    prev_y[...] = jnp.zeros_like(prev_y)
    corner_x[...] = jnp.zeros_like(corner_x)
    corner_y[...] = jnp.zeros_like(corner_y)
    halo_y[...] = jnp.zeros_like(halo_y)
    halo_psi_y[...] = jnp.zeros_like(halo_psi_y)

    barrier = pltpu.get_barrier_semaphore()
    for peer in row_peers:
        pl.semaphore_signal(
            barrier, inc=1, device_id={"row": peer, "col": col}, device_id_type=pl.DeviceIdType.MESH)
    for peer in col_peers:
        pl.semaphore_signal(
            barrier, inc=1, device_id={"row": row, "col": peer}, device_id_type=pl.DeviceIdType.MESH)
    for m in (3, 5):
        @pl.when(routes[m][0])
        def _():
            pl.semaphore_signal(
                barrier, inc=1, device_id=routes[m][1], device_id_type=pl.DeviceIdType.MESH)

    zero = jnp.zeros((nx, ny), jnp.float32)
    for c in range(3):
        e_s[c, nz] = zero
        h_s[c, 0] = zero

    def clear(z, carry):
        for k in range(8):
            psi[k, z] = zero
        return carry

    lax.fori_loop(0, nz, clear, 0)

    sub = lax.broadcasted_iota(jnp.int32, (nx, ny), 0)
    lane = lax.broadcasted_iota(jnp.int32, (nx, ny), 1)
    w = [jnp.full((nx, ny), width_ref[k], jnp.int32).astype(jnp.float32) for k in range(4)]
    x_pos = (sub + row * nx).astype(jnp.float32)
    y_pos = (lane + col * ny).astype(jnp.float32)
    x_before = (jnp.zeros_like(sub) + (row * nx - 1)).astype(jnp.float32)
    y_before = (jnp.zeros_like(sub) + (col * ny - 1)).astype(jnp.float32)
    full_x, full_y = float(nx * n_row), float(ny * n_col)
    pairs = (
        absorber(x_pos + 0.5, full_x, w[0], w[1]), absorber(y_pos + 0.5, full_y, w[2], w[3]),
        absorber(x_pos, full_x, w[0], w[1]), absorber(y_pos, full_y, w[2], w[3]),
        absorber(x_before + 0.5, full_x, w[0], w[1]), absorber(y_before + 0.5, full_y, w[2], w[3]),
    )
    for k, (damp, gain) in enumerate(pairs):
        prof[2 * k] = damp
        prof[2 * k + 1] = gain

    def pack(z, ex, ey, ez, cols):
        first, last0, last1 = cols
        first_x[0, pl.ds(z, 1), :] = ey[0:1]
        first_x[1, pl.ds(z, 1), :] = ez[0:1]
        last_x[0, pl.ds(z, 1), :] = ex[nx - 1:nx]
        last_x[1, pl.ds(z, 1), :] = ey[nx - 1:nx]
        last_x[2, pl.ds(z, 1), :] = ez[nx - 1:nx]
        rx = pltpu.roll(ex, z, 1)
        rz = pltpu.roll(ez, z + nz, 1)
        ry = pltpu.roll(ey, z, 1)
        first = jnp.where(lane == z, rx, jnp.where(lane == z + nz, rz, first))
        before = lax.rem(z + ny - 1, ny)
        last0 = jnp.where(lane == before, rx, jnp.where(lane == z + nz - 1, rz, last0))
        last1 = jnp.where(lane == before, ry, last1)
        return first, last0, last1

    def keep(cols):
        first_y[...] = cols[0]
        last_y[0] = pltpu.roll(cols[1], 1, 1)
        last_y[1] = pltpu.roll(cols[2], 1, 1)

    def copies(slot):
        parts = (
            (first_x, next_x.at[slot]),
            (last_x, prev_x.at[slot, :, pl.ds(0, nz)]),
            (first_y, next_y.at[slot]),
            (first_y, corner_x.at[slot]),
            (last_y, prev_y.at[slot]),
            (last_y.at[1], corner_y.at[slot]),
        )
        return [
            pltpu.make_async_remote_copy(
                src_ref=src, dst_ref=dst, send_sem=send_sem.at[m, slot], recv_sem=recv_sem.at[m, slot],
                device_id=routes[m][1], device_id_type=pl.DeviceIdType.MESH)
            for m, (src, dst) in enumerate(parts)
        ]

    def start_all(slot):
        for m, copy in enumerate(copies(slot)):
            @pl.when(routes[m][0])
            def _():
                copy.start()

    arrives = (down, up, right, ne, left, sw)

    def wait_recv(slot, which):
        every = copies(slot)
        for m in which:
            @pl.when(arrives[m])
            def _():
                every[m].wait_recv()

    def wait_send(slot):
        for m, copy in enumerate(copies(slot)):
            @pl.when(routes[m][0])
            def _():
                copy.wait_send()

    load_e.wait()
    load_h.wait()

    def first_pack(k, carry):
        cols, hcol = carry
        for j in range(UNROLL):
            z = k * UNROLL + j
            cols = pack(z, e_s[0, z], e_s[1, z], e_s[2, z], cols)
            hx, hy, hz = h_s[0, z + 1], h_s[1, z + 1], h_s[2, z + 1]
            h_last_x[0, pl.ds(z, 1), :] = hy[nx - 1:nx]
            h_last_x[1, pl.ds(z, 1), :] = hz[nx - 1:nx]
            hcol = jnp.where(lane == z, pltpu.roll(hz, z + 1, 1), hcol)
            hcol = jnp.where(lane == z + nz, pltpu.roll(hx, lax.rem(z + nz + 1, ny), 1), hcol)
        return cols, hcol

    cols, hcol = lax.fori_loop(0, nz // UNROLL, first_pack, ((zero, zero, zero), zero))
    keep(cols)
    h_last_y[...] = hcol

    count = n_row - 1 + n_col - 1 + sw.astype(jnp.int32) + ne.astype(jnp.int32)
    pl.semaphore_wait(barrier, count)
    once = [
        pltpu.make_async_remote_copy(
            src_ref=src, dst_ref=dst, send_sem=once_send.at[k], recv_sem=once_recv.at[k],
            device_id=routes[m][1], device_id_type=pl.DeviceIdType.MESH)
        for k, (src, dst, m) in enumerate(((h_last_x, halo_x, 1), (h_last_y, halo_y, 4)))
    ]
    start_all(0)
    for k, m in enumerate((1, 4)):
        @pl.when(routes[m][0])
        def _():
            once[k].start()
    load_c.wait()
    piece = n_modes // STEPS

    def mode_copies(s):
        return [
            pltpu.make_async_remote_copy(
                src_ref=basis_in.at[pl.ds(s * piece, piece), pl.ds(pl.multiple_of(peer * nx, nx), nx)],
                dst_ref=modes_3d.at[pl.ds(row * n_modes + s * piece, piece)],
                send_sem=mode_send.at[k, s], recv_sem=mode_recv.at[k, s],
                device_id={"row": peer, "col": col}, device_id_type=pl.DeviceIdType.MESH)
            for k, peer in enumerate(row_peers)
        ]

    def magnetic(slot):
        hdx, hgx, hdy, hgy = prof[0], prof[1], prof[2], prof[3]
        edge = next_y[slot]

        def body(k, carry):
            for j in range(UNROLL):
                z = k * UNROLL + j
                ex, ey, ez = e_s[0, z], e_s[1, z], e_s[2, z]
                row_y = jnp.broadcast_to(next_x[slot, 0, pl.ds(z, 1), :], (nx, ny))
                row_z = jnp.broadcast_to(next_x[slot, 1, pl.ds(z, 1), :], (nx, ny))
                col_x = pltpu.roll(edge, ny - 1 - z, 1)
                col_z = pltpu.roll(edge, ny - 1 - nz - z, 1)
                ey_dz = e_s[1, z + 1] - ey
                ex_dz = e_s[0, z + 1] - ex
                ez_dy = jnp.where(lane == ny - 1, col_z, pltpu.roll(ez, ny - 1, 1)) - ez
                ex_dy = jnp.where(lane == ny - 1, col_x, pltpu.roll(ex, ny - 1, 1)) - ex
                ez_dx = jnp.where(sub == nx - 1, row_z, pltpu.roll(ez, nx - 1, 0)) - ez
                ey_dx = jnp.where(sub == nx - 1, row_y, pltpu.roll(ey, nx - 1, 0)) - ey
                p0 = hdy * psi[0, z] + hgy * ez_dy
                p1 = hdx * psi[1, z] + hgx * ez_dx
                p2 = hdx * psi[2, z] + hgx * ey_dx
                p3 = hdy * psi[3, z] + hgy * ex_dy
                psi[0, z], psi[1, z], psi[2, z], psi[3, z] = p0, p1, p2, p3
                h_s[0, z + 1] = h_s[0, z + 1] - time_step * (ez_dy + p0 - ey_dz)
                h_s[1, z + 1] = h_s[1, z + 1] - time_step * (ex_dz - ez_dx - p1)
                h_s[2, z + 1] = h_s[2, z + 1] - time_step * (ey_dx + p2 - ex_dy - p3)
            return carry

        lax.fori_loop(0, nz // UNROLL, body, 0)

    def magnetic_row_before(slot):
        hdy, hgy = prof[2][0:1], prof[3][0:1]
        hdx, hgx = prof[8][0:1], prof[9][0:1]
        ex, ey, ez = prev_x[slot, 0, 0:nz], prev_x[slot, 1, 0:nz], prev_x[slot, 2, 0:nz]
        big_lane = lax.broadcasted_iota(jnp.int32, (nz, ny), 1)
        big_z = lax.broadcasted_iota(jnp.int32, (nz, ny), 0)
        corner = jnp.broadcast_to(corner_x[slot, nx - 1:nx, :], (nz, ny))
        corner = jnp.sum(jnp.where(big_lane == big_z, corner, 0.0), axis=1, keepdims=True)
        ex_dz = prev_x[slot, 0, 1:nz + 1] - ex
        ex_dy = jnp.where(big_lane == ny - 1, corner, pltpu.roll(ex, ny - 1, 1)) - ex
        ey_dx = first_x[0] - ey
        ez_dx = first_x[1] - ez
        p1 = hdx * halo_psi_x[0] + hgx * ez_dx
        p2 = hdx * halo_psi_x[1] + hgx * ey_dx
        p3 = hdy * halo_psi_x[2] + hgy * ex_dy
        halo_psi_x[0], halo_psi_x[1], halo_psi_x[2] = p1, p2, p3
        mask = up.astype(jnp.float32)
        halo_x[0] = mask * (halo_x[0] - time_step * (ex_dz - ez_dx - p1))
        halo_x[1] = mask * (halo_x[1] - time_step * (ey_dx + p2 - ex_dy - p3))

    def magnetic_column_before(slot):
        hdx, hgx = prof[0], prof[1]
        hdy, hgy = prof[10], prof[11]
        ey = prev_y[slot, 1]
        dy = first_y[...] - prev_y[slot, 0]
        below = jnp.broadcast_to(corner_y[slot, 0:1, :], (nx, ny))
        ey_dx = jnp.where(sub == nx - 1, below, pltpu.roll(ey, nx - 1, 0)) - ey
        ey_dz = pltpu.roll(pltpu.roll(ey, ny - 1, 1) - ey, nz, 1)
        py = hdy * halo_psi_y[0] + hgy * dy
        px = hdx * halo_psi_y[1] + hgx * ey_dx
        halo_psi_y[0], halo_psi_y[1] = py, px
        mask = left.astype(jnp.float32)
        change = jnp.where(lane < nz, ey_dx + px - dy - py, dy + py - ey_dz)
        halo_y[...] = mask * (halo_y[...] - time_step * change)

    def electric():
        edx, egx, edy, egy = prof[4], prof[5], prof[6], prof[7]
        edge = halo_y[...]

        def body(k, cols):
            for j in range(UNROLL):
                z = k * UNROLL + j
                hx, hy, hz = h_s[0, z + 1], h_s[1, z + 1], h_s[2, z + 1]
                row_y = jnp.broadcast_to(halo_x[0, pl.ds(z, 1), :], (nx, ny))
                row_z = jnp.broadcast_to(halo_x[1, pl.ds(z, 1), :], (nx, ny))
                col_z = pltpu.roll(edge, lax.rem(ny - z, ny), 1)
                col_x = pltpu.roll(edge, ny - nz - z, 1)
                hy_dz = hy - h_s[1, z]
                hx_dz = hx - h_s[0, z]
                hz_dy = hz - jnp.where(lane == 0, col_z, pltpu.roll(hz, 1, 1))
                hx_dy = hx - jnp.where(lane == 0, col_x, pltpu.roll(hx, 1, 1))
                hz_dx = hz - jnp.where(sub == 0, row_z, pltpu.roll(hz, 1, 0))
                hy_dx = hy - jnp.where(sub == 0, row_y, pltpu.roll(hy, 1, 0))
                p0 = edy * psi[4, z] + egy * hz_dy
                p1 = edx * psi[5, z] + egx * hz_dx
                p2 = edx * psi[6, z] + egx * hy_dx
                p3 = edy * psi[7, z] + egy * hx_dy
                psi[4, z], psi[5, z], psi[6, z], psi[7, z] = p0, p1, p2, p3
                amount = coef_s[z]
                ex = e_s[0, z] + amount * (hz_dy + p0 - hy_dz)
                ey = e_s[1, z] + amount * (hx_dz - hz_dx - p1)
                ez = e_s[2, z] + amount * (hy_dx + p2 - hx_dy - p3)
                e_s[0, z], e_s[1, z], e_s[2, z] = ex, ey, ez
                cols = pack(z, ex, ey, ez, cols)
            return cols

        keep(lax.fori_loop(0, nz // UNROLL, body, (zero, zero, zero)))

    def step(s, carry):
        slot = lax.rem(s, 2)
        for copy in mode_copies(s):
            copy.start()
        wait_recv(slot, (0, 2))
        magnetic(slot)
        wait_recv(slot, (1, 3))

        @pl.when(s == 0)
        def _():
            for k, there in enumerate((up, left)):
                @pl.when(there)
                def _():
                    once[k].wait_recv()

        magnetic_row_before(slot)
        wait_recv(slot, (4, 5))
        magnetic_column_before(slot)
        wait_send(slot)
        electric()

        @pl.when(s < STEPS - 1)
        def _():
            start_all(1 - slot)

        return carry

    lax.fori_loop(0, STEPS, step, 0)
    for k, m in enumerate((1, 4)):
        @pl.when(routes[m][0])
        def _():
            once[k].wait_send()
    store_e = pltpu.make_async_copy(e_s.at[:, pl.ds(0, nz)], e_out, local_sem.at[0])
    store_h = pltpu.make_async_copy(h_s.at[:, pl.ds(1, nz)], h_out, local_sem.at[1])
    store_e.start()
    store_h.start()

    count = snaps.shape[0] // nx

    def pick(s, carry):
        index = index_ref[s]
        c = index // nz
        z = index - c * nz + (c // 3)
        snaps[pl.ds(pl.multiple_of(s * nx, nx), nx), :] = fields[c, z]
        return carry

    lax.fori_loop(0, count, pick, 0)
    load_b.wait()

    def wait_modes(s, carry):
        for copy in mode_copies(s):
            copy.wait()
        return carry

    lax.fori_loop(0, STEPS, wait_modes, 0)
    n_all = modes.shape[0] // nx
    dims = (((1,), (1,)), ((), ()))
    proj, gram = None, None
    for x in range(nx):
        a = snaps[pl.ds(x, count, stride=nx), :]
        b = modes[pl.ds(x, n_all, stride=nx), :]
        p = lax.dot_general(a, b, dims, precision=lax.Precision.HIGHEST, preferred_element_type=jnp.float32)
        g = lax.dot_general(a, a, dims, precision=lax.Precision.HIGHEST, preferred_element_type=jnp.float32)
        proj, gram = (p, g) if x == 0 else (proj + p, gram + g)
    part[:, 0:n_all] = proj
    part[:, n_all:n_all + count] = gram / float(nx * n_row * ny * n_col)

    share = count // n_row
    own = pl.ds(pl.multiple_of(row * share, share), share)

    def exchange(peers, axis, src_of, dst, sends, recvs):
        result = []
        for k, peer in enumerate(peers):
            where = {"row": row, "col": col}
            where[axis] = peer
            result.append(pltpu.make_async_remote_copy(
                src_ref=src_of(peer), dst_ref=dst, send_sem=sends.at[k], recv_sem=recvs.at[k],
                device_id=where, device_id_type=pl.DeviceIdType.MESH))
        for copy in result:
            copy.start()
        for copy in result:
            copy.wait()

    row_sums[row] = part[own, :]
    exchange(
        row_peers, "row", lambda peer: part.at[pl.ds(pl.multiple_of(peer * share, share), share)],
        row_sums.at[row], sum_send, sum_recv)
    value = row_sums[0]
    for k in range(1, n_row):
        value = value + row_sums[k]
    col_sums[col] = value
    exchange(col_peers, "col", lambda peer: col_sums.at[col], col_sums.at[col], col_send, col_recv)
    value = col_sums[0]
    for k in range(1, n_col):
        value = value + col_sums[k]
    total[own, :] = value
    exchange(row_peers, "row", lambda peer: total.at[own], total.at[own], back_send, back_recv)
    proj_out[...] = total[:, 0:n_all]
    gram_out[...] = total[:, n_all:n_all + count]
    store_e.wait()
    store_h.wait()


def shards(e_field, h_field, e_coef, basis, pml_width, snap_index):
    nz, nx, ny = e_coef.shape
    n_row, n_col = lax.axis_size("row"), lax.axis_size("col")
    modes, count = basis.shape[0] * n_row, snap_index.shape[0]
    f32 = jnp.float32
    wide = modes + (count + 127) // 128 * 128
    any_space = pl.BlockSpec(memory_space=pl.ANY)
    smem, vmem = pl.BlockSpec(memory_space=pltpu.SMEM), pl.BlockSpec(memory_space=pltpu.VMEM)
    return pl.pallas_call(
        functools.partial(step_kernel, n_row, n_col),
        out_shape=[
            jax.ShapeDtypeStruct(e_field.shape, f32), jax.ShapeDtypeStruct(h_field.shape, f32),
            jax.ShapeDtypeStruct((count, modes), f32), jax.ShapeDtypeStruct((count, count), f32),
        ],
        in_specs=[smem, smem, any_space, any_space, any_space, any_space],
        out_specs=[any_space, any_space, vmem, vmem],
        scratch_shapes=[
            pltpu.VMEM((6, nz + 1, nx, ny), f32),
            pltpu.VMEM((nz, nx, ny), f32), pltpu.VMEM((8, nz, nx, ny), f32),
            pltpu.VMEM((2, nz, ny), f32), pltpu.VMEM((3, nz, ny), f32), pltpu.VMEM((2, nz, ny), f32),
            pltpu.VMEM((nx, ny), f32), pltpu.VMEM((2, nx, ny), f32), pltpu.VMEM((nx, ny), f32),
            pltpu.VMEM((2, 2, nz, ny), f32), pltpu.VMEM((2, 3, nz + 8, ny), f32),
            pltpu.VMEM((2, nz, ny), f32), pltpu.VMEM((3, nz, ny), f32),
            pltpu.VMEM((2, nx, ny), f32), pltpu.VMEM((2, 2, nx, ny), f32),
            pltpu.VMEM((2, nx, ny), f32), pltpu.VMEM((2, nx, ny), f32),
            pltpu.VMEM((nx, ny), f32), pltpu.VMEM((2, nx, ny), f32),
            pltpu.VMEM((12, nx, ny), f32),
            pltpu.VMEM((modes * nx, ny), f32), pltpu.VMEM((count * nx, ny), f32),
            pltpu.VMEM((count, wide), f32), pltpu.VMEM((n_row, count // n_row, wide), f32),
            pltpu.VMEM((n_col, count // n_row, wide), f32), pltpu.VMEM((count, wide), f32),
            pltpu.SemaphoreType.DMA((4,)),
            pltpu.SemaphoreType.DMA((6, 2)), pltpu.SemaphoreType.DMA((6, 2)),
            pltpu.SemaphoreType.DMA((2,)), pltpu.SemaphoreType.DMA((2,)),
            pltpu.SemaphoreType.DMA((n_row - 1, STEPS)), pltpu.SemaphoreType.DMA((n_row - 1, STEPS)),
            pltpu.SemaphoreType.DMA((n_row - 1,)), pltpu.SemaphoreType.DMA((n_row - 1,)),
            pltpu.SemaphoreType.DMA((n_col - 1,)), pltpu.SemaphoreType.DMA((n_col - 1,)),
            pltpu.SemaphoreType.DMA((n_row - 1,)), pltpu.SemaphoreType.DMA((n_row - 1,)),
        ],
        compiler_params=pltpu.CompilerParams(
            collective_id=0, has_side_effects=True, vmem_limit_bytes=32 * 1024 * 1024
        ),
    )(pml_width, snap_index, e_field, h_field, e_coef, basis)


def solution(mesh):
    in_specs = (
        P(None, None, "row", "col"),
        P(None, None, "row", "col"),
        P(None, "row", "col"),
        P("row", None, "col"),
        P(),
        P(),
    )
    out_specs = (P(None, None, "row", "col"), P(None, None, "row", "col"), P(), P())
    return jax.shard_map(shards, mesh=mesh, in_specs=in_specs, out_specs=out_specs, check_vma=False)
```

```python
import functools
import jax
import jax.numpy as jnp
from jax import lax
from jax.experimental import pallas as pl
from jax.experimental.pallas import tpu as pltpu
from jax.sharding import PartitionSpec as P

STEPS = 8
UNROLL = 16

time_step = 0.5
sigma_top = 4.0
alpha_shift = 0.05


def absorber(positions, total, low, high):
    depth = jnp.maximum(
        jnp.maximum((low - positions) / low, (positions - (total - 1.0 - high)) / high), 0.0
    )
    sigma = sigma_top * (depth * depth * depth)
    damp = jnp.exp(-(sigma + alpha_shift) * time_step)
    gain = sigma / (sigma + alpha_shift) * (damp - 1.0)
    return damp, gain


def step_kernel(
    n_row, n_col, width_ref, index_ref, e_in, h_in, coef_in, basis_in, e_out, h_out, proj_out, gram_out,
    fields, coef_s, psi, first_x, last_x, h_last_x, first_y, last_y, h_last_y,
    next_x, prev_x, halo_x, halo_psi_x, next_y, prev_y, corner_x, corner_y, halo_y, halo_psi_y,
    prof, modes, snaps, part, row_sums, col_sums, total,
    local_sem, x_send, x_recv, send_sem, recv_sem, once_send, once_recv, mode_send, mode_recv,
    sum_send, sum_recv, col_send, col_recv, back_send, back_recv,
):
    e_s, h_s = fields.at[pl.ds(0, 3)], fields.at[pl.ds(3, 3)]
    nz, nx, ny = coef_s.shape
    row, col = lax.axis_index("row"), lax.axis_index("col")
    up, down = row > 0, row < n_row - 1
    left, right = col > 0, col < n_col - 1
    sw = jnp.logical_and(down, left)
    ne = jnp.logical_and(up, right)
    routes = (
        (up, {"row": row - 1, "col": col}), (down, {"row": row + 1, "col": col}),
        (left, {"row": row, "col": col - 1}), (sw, {"row": row + 1, "col": col - 1}),
        (right, {"row": row, "col": col + 1}), (ne, {"row": row - 1, "col": col + 1}),
        (left, {"row": row, "col": col - 1}),
    )
    chunks = nz // UNROLL
    half = chunks // 2

    load_e = pltpu.make_async_copy(e_in, e_s.at[:, pl.ds(0, nz)], local_sem.at[0])
    load_h = pltpu.make_async_copy(h_in, h_s.at[:, pl.ds(1, nz)], local_sem.at[1])
    load_c = pltpu.make_async_copy(coef_in, coef_s, local_sem.at[2])
    load_e.start()
    load_h.start()
    load_c.start()
    n_modes = basis_in.shape[0]
    modes_3d = modes.reshape(n_modes * n_row, nx, ny)
    load_b = pltpu.make_async_copy(
        basis_in.at[:, pl.ds(pl.multiple_of(row * nx, nx), nx)],
        modes_3d.at[pl.ds(row * n_modes, n_modes)], local_sem.at[3])
    load_b.start()
    row_peers = [lax.rem(row + k, n_row) for k in range(1, n_row)]
    col_peers = [lax.rem(col + k, n_col) for k in range(1, n_col)]

    part[...] = jnp.zeros_like(part)
    next_x[...] = jnp.zeros_like(next_x)
    prev_x[...] = jnp.zeros_like(prev_x)
    halo_x[...] = jnp.zeros_like(halo_x)
    halo_psi_x[...] = jnp.zeros_like(halo_psi_x)
    next_y[...] = jnp.zeros_like(next_y)
    prev_y[...] = jnp.zeros_like(prev_y)
    corner_x[...] = jnp.zeros_like(corner_x)
    corner_y[...] = jnp.zeros_like(corner_y)
    halo_y[...] = jnp.zeros_like(halo_y)
    halo_psi_y[...] = jnp.zeros_like(halo_psi_y)

    barrier = pltpu.get_barrier_semaphore()
    for peer in row_peers:
        pl.semaphore_signal(
            barrier, inc=1, device_id={"row": peer, "col": col}, device_id_type=pl.DeviceIdType.MESH)
    for peer in col_peers:
        pl.semaphore_signal(
            barrier, inc=1, device_id={"row": row, "col": peer}, device_id_type=pl.DeviceIdType.MESH)
    for m in (3, 5):
        @pl.when(routes[m][0])
        def _():
            pl.semaphore_signal(
                barrier, inc=1, device_id=routes[m][1], device_id_type=pl.DeviceIdType.MESH)

    zero = jnp.zeros((nx, ny), jnp.float32)
    for c in range(3):
        e_s[c, nz] = zero
        h_s[c, 0] = zero

    def clear(z, carry):
        for k in range(8):
            psi[k, z] = zero
        return carry

    lax.fori_loop(0, nz, clear, 0)

    sub = lax.broadcasted_iota(jnp.int32, (nx, ny), 0)
    lane = lax.broadcasted_iota(jnp.int32, (nx, ny), 1)
    w = [jnp.full((nx, ny), width_ref[k], jnp.int32).astype(jnp.float32) for k in range(4)]
    x_pos = (sub + row * nx).astype(jnp.float32)
    y_pos = (lane + col * ny).astype(jnp.float32)
    x_before = (jnp.zeros_like(sub) + (row * nx - 1)).astype(jnp.float32)
    y_before = (jnp.zeros_like(sub) + (col * ny - 1)).astype(jnp.float32)
    full_x, full_y = float(nx * n_row), float(ny * n_col)
    pairs = (
        absorber(x_pos + 0.5, full_x, w[0], w[1]), absorber(y_pos + 0.5, full_y, w[2], w[3]),
        absorber(x_pos, full_x, w[0], w[1]), absorber(y_pos, full_y, w[2], w[3]),
        absorber(x_before + 0.5, full_x, w[0], w[1]), absorber(y_before + 0.5, full_y, w[2], w[3]),
    )
    for k, (damp, gain) in enumerate(pairs):
        prof[2 * k] = damp
        prof[2 * k + 1] = gain

    def pack(z, ex, ey, ez, cols):
        first, last0, last1 = cols
        first_x[0, pl.ds(z, 1), :] = ey[0:1]
        first_x[1, pl.ds(z, 1), :] = ez[0:1]
        last_x[0, pl.ds(z, 1), :] = ex[nx - 1:nx]
        last_x[1, pl.ds(z, 1), :] = ey[nx - 1:nx]
        last_x[2, pl.ds(z, 1), :] = ez[nx - 1:nx]
        rx = pltpu.roll(ex, z, 1)
        rz = pltpu.roll(ez, z + nz, 1)
        ry = pltpu.roll(ey, z, 1)
        first = jnp.where(lane == z, rx, jnp.where(lane == z + nz, rz, first))
        before = lax.rem(z + ny - 1, ny)
        last0 = jnp.where(lane == before, rx, jnp.where(lane == z + nz - 1, rz, last0))
        last1 = jnp.where(lane == before, ry, last1)
        return first, last0, last1

    def keep(cols):
        first_y[1] = cols[0]
        last_y[0] = pltpu.roll(cols[1], 1, 1)
        last_y[1] = pltpu.roll(cols[2], 1, 1)

    def remote(m, src, dst, send, recv):
        return pltpu.make_async_remote_copy(
            src_ref=src, dst_ref=dst, send_sem=send, recv_sem=recv,
            device_id=routes[m][1], device_id_type=pl.DeviceIdType.MESH)

    def copy_of(m, slot, k=None):
        if m < 2:
            here = pl.ds(pl.multiple_of(k * UNROLL, UNROLL), UNROLL)
            src, dst = ((first_x, next_x), (last_x, prev_x))[m]
            return remote(
                m, src.at[:, here], dst.at[slot, :, here], x_send.at[m, slot, k], x_recv.at[m, slot, k])
        src, dst = {
            2: (first_y.at[1], next_y.at[slot, 1]), 3: (first_y.at[1], corner_x.at[slot]),
            4: (last_y, prev_y.at[slot]), 5: (last_y.at[1], corner_y.at[slot]),
            6: (first_y.at[0], next_y.at[slot, 0]),
        }[m]
        return remote(m, src, dst, send_sem.at[m, slot], recv_sem.at[m, slot])

    def start(m, slot, k=None):
        @pl.when(routes[m][0])
        def _():
            copy_of(m, slot, k).start()

    arrives = (down, up, right, ne, left, sw, right)

    def wait_recv(m, slot, k=None):
        @pl.when(arrives[m])
        def _():
            copy_of(m, slot, k).wait_recv()

    def wait_send(m, slot, k=None):
        @pl.when(routes[m][0])
        def _():
            copy_of(m, slot, k).wait_send()

    load_e.wait()
    load_h.wait()

    def first_pack(k, carry):
        cols, hcol = carry
        for j in range(UNROLL):
            z = k * UNROLL + j
            cols = pack(z, e_s[0, z], e_s[1, z], e_s[2, z], cols)
            hx, hy, hz = h_s[0, z + 1], h_s[1, z + 1], h_s[2, z + 1]
            h_last_x[0, pl.ds(z, 1), :] = hy[nx - 1:nx]
            h_last_x[1, pl.ds(z, 1), :] = hz[nx - 1:nx]
            hcol = jnp.where(lane == z, pltpu.roll(hz, z + 1, 1), hcol)
            hcol = jnp.where(lane == z + nz, pltpu.roll(hx, lax.rem(z + nz + 1, ny), 1), hcol)
        return cols, hcol

    cols, hcol = lax.fori_loop(0, nz // UNROLL, first_pack, ((zero, zero, zero), zero))
    keep(cols)
    first_y[0] = cols[0]
    h_last_y[...] = hcol

    count = n_row - 1 + n_col - 1 + sw.astype(jnp.int32) + ne.astype(jnp.int32)
    pl.semaphore_wait(barrier, count)
    once = [
        pltpu.make_async_remote_copy(
            src_ref=src, dst_ref=dst, send_sem=once_send.at[k], recv_sem=once_recv.at[k],
            device_id=routes[m][1], device_id_type=pl.DeviceIdType.MESH)
        for k, (src, dst, m) in enumerate(((h_last_x, halo_x, 1), (h_last_y, halo_y, 4)))
    ]
    for k in range(chunks):
        start(0, 0, k)
        start(1, 0, k)
    for m in (2, 4, 6, 3, 5):
        start(m, 0)
    for k, m in enumerate((1, 4)):
        @pl.when(routes[m][0])
        def _():
            once[k].start()
    load_c.wait()
    piece = n_modes // STEPS

    def mode_copies(s):
        return [
            pltpu.make_async_remote_copy(
                src_ref=basis_in.at[pl.ds(s * piece, piece), pl.ds(pl.multiple_of(peer * nx, nx), nx)],
                dst_ref=modes_3d.at[pl.ds(row * n_modes + s * piece, piece)],
                send_sem=mode_send.at[k, s], recv_sem=mode_recv.at[k, s],
                device_id={"row": peer, "col": col}, device_id_type=pl.DeviceIdType.MESH)
            for k, peer in enumerate(row_peers)
        ]

    def magnetic(slot):
        hdx, hgx, hdy, hgy = prof[0], prof[1], prof[2], prof[3]

        def body(k, carry):
            wait_recv(0, slot, k)

            @pl.when(k == 0)
            def _():
                wait_recv(6, slot)

            @pl.when(k == half)
            def _():
                wait_recv(2, slot)

            edge = next_y[slot, k // half]
            for j in range(UNROLL):
                z = k * UNROLL + j
                ex, ey, ez = e_s[0, z], e_s[1, z], e_s[2, z]
                row_y = jnp.broadcast_to(next_x[slot, 0, pl.ds(z, 1), :], (nx, ny))
                row_z = jnp.broadcast_to(next_x[slot, 1, pl.ds(z, 1), :], (nx, ny))
                col_x = pltpu.roll(edge, ny - 1 - z, 1)
                col_z = pltpu.roll(edge, ny - 1 - nz - z, 1)
                ey_dz = e_s[1, z + 1] - ey
                ex_dz = e_s[0, z + 1] - ex
                ez_dy = jnp.where(lane == ny - 1, col_z, pltpu.roll(ez, ny - 1, 1)) - ez
                ex_dy = jnp.where(lane == ny - 1, col_x, pltpu.roll(ex, ny - 1, 1)) - ex
                ez_dx = jnp.where(sub == nx - 1, row_z, pltpu.roll(ez, nx - 1, 0)) - ez
                ey_dx = jnp.where(sub == nx - 1, row_y, pltpu.roll(ey, nx - 1, 0)) - ey
                p0 = hdy * psi[0, z] + hgy * ez_dy
                p1 = hdx * psi[1, z] + hgx * ez_dx
                p2 = hdx * psi[2, z] + hgx * ey_dx
                p3 = hdy * psi[3, z] + hgy * ex_dy
                psi[0, z], psi[1, z], psi[2, z], psi[3, z] = p0, p1, p2, p3
                h_s[0, z + 1] = h_s[0, z + 1] - time_step * (ez_dy + p0 - ey_dz)
                h_s[1, z + 1] = h_s[1, z + 1] - time_step * (ex_dz - ez_dx - p1)
                h_s[2, z + 1] = h_s[2, z + 1] - time_step * (ey_dx + p2 - ex_dy - p3)
            return carry

        lax.fori_loop(0, nz // UNROLL, body, 0)

    def magnetic_row_before(slot):
        hdy, hgy = prof[2][0:1], prof[3][0:1]
        hdx, hgx = prof[8][0:1], prof[9][0:1]
        ex, ey, ez = prev_x[slot, 0, 0:nz], prev_x[slot, 1, 0:nz], prev_x[slot, 2, 0:nz]
        big_lane = lax.broadcasted_iota(jnp.int32, (nz, ny), 1)
        big_z = lax.broadcasted_iota(jnp.int32, (nz, ny), 0)
        corner = jnp.broadcast_to(corner_x[slot, nx - 1:nx, :], (nz, ny))
        corner = jnp.sum(jnp.where(big_lane == big_z, corner, 0.0), axis=1, keepdims=True)
        ex_dz = prev_x[slot, 0, 1:nz + 1] - ex
        ex_dy = jnp.where(big_lane == ny - 1, corner, pltpu.roll(ex, ny - 1, 1)) - ex
        ey_dx = first_x[0] - ey
        ez_dx = first_x[1] - ez
        p1 = hdx * halo_psi_x[0] + hgx * ez_dx
        p2 = hdx * halo_psi_x[1] + hgx * ey_dx
        p3 = hdy * halo_psi_x[2] + hgy * ex_dy
        halo_psi_x[0], halo_psi_x[1], halo_psi_x[2] = p1, p2, p3
        mask = up.astype(jnp.float32)
        halo_x[0] = mask * (halo_x[0] - time_step * (ex_dz - ez_dx - p1))
        halo_x[1] = mask * (halo_x[1] - time_step * (ey_dx + p2 - ex_dy - p3))

    def magnetic_column_before(slot):
        hdx, hgx = prof[0], prof[1]
        hdy, hgy = prof[10], prof[11]
        ey = prev_y[slot, 1]
        dy = first_y[1] - prev_y[slot, 0]
        below = jnp.broadcast_to(corner_y[slot, 0:1, :], (nx, ny))
        ey_dx = jnp.where(sub == nx - 1, below, pltpu.roll(ey, nx - 1, 0)) - ey
        ey_dz = pltpu.roll(pltpu.roll(ey, ny - 1, 1) - ey, nz, 1)
        py = hdy * halo_psi_y[0] + hgy * dy
        px = hdx * halo_psi_y[1] + hgx * ey_dx
        halo_psi_y[0], halo_psi_y[1] = py, px
        mask = left.astype(jnp.float32)
        change = jnp.where(lane < nz, ey_dx + px - dy - py, dy + py - ey_dz)
        halo_y[...] = mask * (halo_y[...] - time_step * change)

    def electric(s, slot):
        edx, egx, edy, egy = prof[4], prof[5], prof[6], prof[7]
        edge = halo_y[...]

        def body(k, cols):
            for j in range(UNROLL):
                z = k * UNROLL + j
                hx, hy, hz = h_s[0, z + 1], h_s[1, z + 1], h_s[2, z + 1]
                row_y = jnp.broadcast_to(halo_x[0, pl.ds(z, 1), :], (nx, ny))
                row_z = jnp.broadcast_to(halo_x[1, pl.ds(z, 1), :], (nx, ny))
                col_z = pltpu.roll(edge, lax.rem(ny - z, ny), 1)
                col_x = pltpu.roll(edge, ny - nz - z, 1)
                hy_dz = hy - h_s[1, z]
                hx_dz = hx - h_s[0, z]
                hz_dy = hz - jnp.where(lane == 0, col_z, pltpu.roll(hz, 1, 1))
                hx_dy = hx - jnp.where(lane == 0, col_x, pltpu.roll(hx, 1, 1))
                hz_dx = hz - jnp.where(sub == 0, row_z, pltpu.roll(hz, 1, 0))
                hy_dx = hy - jnp.where(sub == 0, row_y, pltpu.roll(hy, 1, 0))
                p0 = edy * psi[4, z] + egy * hz_dy
                p1 = edx * psi[5, z] + egx * hz_dx
                p2 = edx * psi[6, z] + egx * hy_dx
                p3 = edy * psi[7, z] + egy * hx_dy
                psi[4, z], psi[5, z], psi[6, z], psi[7, z] = p0, p1, p2, p3
                amount = coef_s[z]
                ex = e_s[0, z] + amount * (hz_dy + p0 - hy_dz)
                ey = e_s[1, z] + amount * (hx_dz - hz_dx - p1)
                ez = e_s[2, z] + amount * (hy_dx + p2 - hx_dy - p3)
                e_s[0, z], e_s[1, z], e_s[2, z] = ex, ey, ez
                cols = pack(z, ex, ey, ez, cols)
            more = s < STEPS - 1

            @pl.when(more)
            def _():
                start(0, slot, k)
                start(1, slot, k)

            @pl.when(k == half - 1)
            def _():
                first_y[0] = cols[0]

                @pl.when(more)
                def _():
                    start(6, slot)

            return cols

        keep(lax.fori_loop(0, nz // UNROLL, body, (zero, zero, zero)))

    def step(s, carry):
        slot = lax.rem(s, 2)
        for copy in mode_copies(s):
            copy.start()
        magnetic(slot)
        for k in range(chunks):
            wait_recv(1, slot, k)
        wait_recv(3, slot)

        @pl.when(s == 0)
        def _():
            for k, there in enumerate((up, left)):
                @pl.when(there)
                def _():
                    once[k].wait_recv()

        magnetic_row_before(slot)
        wait_recv(4, slot)
        wait_recv(5, slot)
        magnetic_column_before(slot)
        for k in range(chunks):
            wait_send(0, slot, k)
            wait_send(1, slot, k)
        for m in range(2, 7):
            wait_send(m, slot)
        electric(s, 1 - slot)

        @pl.when(s < STEPS - 1)
        def _():
            for m in (2, 4, 3, 5):
                start(m, 1 - slot)

        return carry

    lax.fori_loop(0, STEPS, step, 0)
    for k, m in enumerate((1, 4)):
        @pl.when(routes[m][0])
        def _():
            once[k].wait_send()
    store_e = pltpu.make_async_copy(e_s.at[:, pl.ds(0, nz)], e_out, local_sem.at[0])
    store_h = pltpu.make_async_copy(h_s.at[:, pl.ds(1, nz)], h_out, local_sem.at[1])
    store_e.start()
    store_h.start()

    count = snaps.shape[0] // nx

    def pick(s, carry):
        index = index_ref[s]
        c = index // nz
        z = index - c * nz + (c // 3)
        snaps[pl.ds(pl.multiple_of(s * nx, nx), nx), :] = fields[c, z]
        return carry

    lax.fori_loop(0, count, pick, 0)
    load_b.wait()

    def wait_modes(s, carry):
        for copy in mode_copies(s):
            copy.wait()
        return carry

    lax.fori_loop(0, STEPS, wait_modes, 0)
    n_all = modes.shape[0] // nx
    dims = (((1,), (1,)), ((), ()))
    proj, gram = None, None
    for x in range(nx):
        a = snaps[pl.ds(x, count, stride=nx), :]
        b = modes[pl.ds(x, n_all, stride=nx), :]
        p = lax.dot_general(a, b, dims, precision=lax.Precision.HIGHEST, preferred_element_type=jnp.float32)
        g = lax.dot_general(a, a, dims, precision=lax.Precision.HIGHEST, preferred_element_type=jnp.float32)
        proj, gram = (p, g) if x == 0 else (proj + p, gram + g)
    part[:, 0:n_all] = proj
    part[:, n_all:n_all + count] = gram / float(nx * n_row * ny * n_col)

    share = count // n_row
    own = pl.ds(pl.multiple_of(row * share, share), share)

    def exchange(peers, axis, src_of, dst, sends, recvs):
        result = []
        for k, peer in enumerate(peers):
            where = {"row": row, "col": col}
            where[axis] = peer
            result.append(pltpu.make_async_remote_copy(
                src_ref=src_of(peer), dst_ref=dst, send_sem=sends.at[k], recv_sem=recvs.at[k],
                device_id=where, device_id_type=pl.DeviceIdType.MESH))
        for copy in result:
            copy.start()
        for copy in result:
            copy.wait()

    row_sums[row] = part[own, :]
    exchange(
        row_peers, "row", lambda peer: part.at[pl.ds(pl.multiple_of(peer * share, share), share)],
        row_sums.at[row], sum_send, sum_recv)
    value = row_sums[0]
    for k in range(1, n_row):
        value = value + row_sums[k]
    col_sums[col] = value
    exchange(col_peers, "col", lambda peer: col_sums.at[col], col_sums.at[col], col_send, col_recv)
    value = col_sums[0]
    for k in range(1, n_col):
        value = value + col_sums[k]
    total[own, :] = value
    exchange(row_peers, "row", lambda peer: total.at[own], total.at[own], back_send, back_recv)
    proj_out[...] = total[:, 0:n_all]
    gram_out[...] = total[:, n_all:n_all + count]
    store_e.wait()
    store_h.wait()


def shards(e_field, h_field, e_coef, basis, pml_width, snap_index):
    nz, nx, ny = e_coef.shape
    n_row, n_col = lax.axis_size("row"), lax.axis_size("col")
    modes, count = basis.shape[0] * n_row, snap_index.shape[0]
    f32 = jnp.float32
    wide = modes + (count + 127) // 128 * 128
    any_space = pl.BlockSpec(memory_space=pl.ANY)
    smem, vmem = pl.BlockSpec(memory_space=pltpu.SMEM), pl.BlockSpec(memory_space=pltpu.VMEM)
    return pl.pallas_call(
        functools.partial(step_kernel, n_row, n_col),
        out_shape=[
            jax.ShapeDtypeStruct(e_field.shape, f32), jax.ShapeDtypeStruct(h_field.shape, f32),
            jax.ShapeDtypeStruct((count, modes), f32), jax.ShapeDtypeStruct((count, count), f32),
        ],
        in_specs=[smem, smem, any_space, any_space, any_space, any_space],
        out_specs=[any_space, any_space, vmem, vmem],
        scratch_shapes=[
            pltpu.VMEM((6, nz + 1, nx, ny), f32),
            pltpu.VMEM((nz, nx, ny), f32), pltpu.VMEM((8, nz, nx, ny), f32),
            pltpu.VMEM((2, nz, ny), f32), pltpu.VMEM((3, nz, ny), f32), pltpu.VMEM((2, nz, ny), f32),
            pltpu.VMEM((2, nx, ny), f32), pltpu.VMEM((2, nx, ny), f32), pltpu.VMEM((nx, ny), f32),
            pltpu.VMEM((2, 2, nz, ny), f32), pltpu.VMEM((2, 3, nz + 8, ny), f32),
            pltpu.VMEM((2, nz, ny), f32), pltpu.VMEM((3, nz, ny), f32),
            pltpu.VMEM((2, 2, nx, ny), f32), pltpu.VMEM((2, 2, nx, ny), f32),
            pltpu.VMEM((2, nx, ny), f32), pltpu.VMEM((2, nx, ny), f32),
            pltpu.VMEM((nx, ny), f32), pltpu.VMEM((2, nx, ny), f32),
            pltpu.VMEM((12, nx, ny), f32),
            pltpu.VMEM((modes * nx, ny), f32), pltpu.VMEM((count * nx, ny), f32),
            pltpu.VMEM((count, wide), f32), pltpu.VMEM((n_row, count // n_row, wide), f32),
            pltpu.VMEM((n_col, count // n_row, wide), f32), pltpu.VMEM((count, wide), f32),
            pltpu.SemaphoreType.DMA((4,)),
            pltpu.SemaphoreType.DMA((2, 2, nz // UNROLL)), pltpu.SemaphoreType.DMA((2, 2, nz // UNROLL)),
            pltpu.SemaphoreType.DMA((7, 2)), pltpu.SemaphoreType.DMA((7, 2)),
            pltpu.SemaphoreType.DMA((2,)), pltpu.SemaphoreType.DMA((2,)),
            pltpu.SemaphoreType.DMA((n_row - 1, STEPS)), pltpu.SemaphoreType.DMA((n_row - 1, STEPS)),
            pltpu.SemaphoreType.DMA((n_row - 1,)), pltpu.SemaphoreType.DMA((n_row - 1,)),
            pltpu.SemaphoreType.DMA((n_col - 1,)), pltpu.SemaphoreType.DMA((n_col - 1,)),
            pltpu.SemaphoreType.DMA((n_row - 1,)), pltpu.SemaphoreType.DMA((n_row - 1,)),
        ],
        compiler_params=pltpu.CompilerParams(
            collective_id=0, has_side_effects=True, vmem_limit_bytes=67_043_328
        ),
    )(pml_width, snap_index, e_field, h_field, e_coef, basis)


def solution(mesh):
    in_specs = (
        P(None, None, "row", "col"),
        P(None, None, "row", "col"),
        P(None, "row", "col"),
        P("row", None, "col"),
        P(),
        P(),
    )
    out_specs = (P(None, None, "row", "col"), P(None, None, "row", "col"), P(), P())
    return jax.shard_map(shards, mesh=mesh, in_specs=in_specs, out_specs=out_specs, check_vma=False)
```

```python
import functools
import jax
import jax.numpy as jnp
from jax import lax
from jax.experimental import pallas as pl
from jax.experimental.pallas import tpu as pltpu
from jax.sharding import PartitionSpec as P

STEPS = 8
UNROLL = 16

time_step = 0.5
sigma_top = 4.0
alpha_shift = 0.05


def absorber(positions, total, low, high):
    depth = jnp.maximum(
        jnp.maximum((low - positions) / low, (positions - (total - 1.0 - high)) / high), 0.0
    )
    sigma = sigma_top * (depth * depth * depth)
    damp = jnp.exp(-(sigma + alpha_shift) * time_step)
    gain = sigma / (sigma + alpha_shift) * (damp - 1.0)
    return damp, gain


def step_kernel(
    n_row, n_col, width_ref, index_ref, e_in, h_in, coef_in, basis_in, e_out, h_out, proj_out, gram_out,
    fields, coef_s, psi, first_x, last_x, h_last_x, first_y, last_y, h_last_y,
    next_x, prev_x, halo_x, halo_psi_x, next_y, prev_y, corner_x, corner_y, halo_y, halo_psi_y,
    prof, modes, snaps, part, row_sums, col_sums, total,
    local_sem, x_send, x_recv, send_sem, recv_sem, once_send, once_recv, mode_send, mode_recv,
    sum_send, sum_recv, col_send, col_recv, back_send, back_recv,
):
    e_s, h_s = fields.at[pl.ds(0, 3)], fields.at[pl.ds(3, 3)]
    nz, nx, ny = coef_s.shape
    row, col = lax.axis_index("row"), lax.axis_index("col")
    up, down = row > 0, row < n_row - 1
    left, right = col > 0, col < n_col - 1
    sw = jnp.logical_and(down, left)
    ne = jnp.logical_and(up, right)
    routes = (
        (up, {"row": row - 1, "col": col}), (down, {"row": row + 1, "col": col}),
        (left, {"row": row, "col": col - 1}), (sw, {"row": row + 1, "col": col - 1}),
        (right, {"row": row, "col": col + 1}), (ne, {"row": row - 1, "col": col + 1}),
        (left, {"row": row, "col": col - 1}),
    )
    chunks = nz // UNROLL
    half = chunks // 2

    load_e = pltpu.make_async_copy(e_in, e_s.at[:, pl.ds(0, nz)], local_sem.at[0])
    load_h = pltpu.make_async_copy(h_in, h_s.at[:, pl.ds(1, nz)], local_sem.at[1])
    load_c = pltpu.make_async_copy(coef_in, coef_s, local_sem.at[2])
    load_e.start()
    load_h.start()
    load_c.start()
    n_modes = basis_in.shape[0]
    modes_3d = modes.reshape(n_modes * n_row, nx, ny)
    load_b = pltpu.make_async_copy(
        basis_in.at[:, pl.ds(pl.multiple_of(row * nx, nx), nx)],
        modes_3d.at[pl.ds(row * n_modes, n_modes)], local_sem.at[3])
    load_b.start()
    row_peers = [lax.rem(row + k, n_row) for k in range(1, n_row)]
    col_peers = [lax.rem(col + k, n_col) for k in range(1, n_col)]

    part[...] = jnp.zeros_like(part)
    next_x[...] = jnp.zeros_like(next_x)
    prev_x[...] = jnp.zeros_like(prev_x)
    halo_x[...] = jnp.zeros_like(halo_x)
    halo_psi_x[...] = jnp.zeros_like(halo_psi_x)
    next_y[...] = jnp.zeros_like(next_y)
    prev_y[...] = jnp.zeros_like(prev_y)
    corner_x[...] = jnp.zeros_like(corner_x)
    corner_y[...] = jnp.zeros_like(corner_y)
    halo_y[...] = jnp.zeros_like(halo_y)
    halo_psi_y[...] = jnp.zeros_like(halo_psi_y)

    barrier = pltpu.get_barrier_semaphore()
    for peer in row_peers:
        pl.semaphore_signal(
            barrier, inc=1, device_id={"row": peer, "col": col}, device_id_type=pl.DeviceIdType.MESH)
    for peer in col_peers:
        pl.semaphore_signal(
            barrier, inc=1, device_id={"row": row, "col": peer}, device_id_type=pl.DeviceIdType.MESH)
    for m in (3, 5):
        @pl.when(routes[m][0])
        def _():
            pl.semaphore_signal(
                barrier, inc=1, device_id=routes[m][1], device_id_type=pl.DeviceIdType.MESH)

    zero = jnp.zeros((nx, ny), jnp.float32)
    for c in range(3):
        e_s[c, nz] = zero
        h_s[c, 0] = zero

    def clear(z, carry):
        for k in range(8):
            psi[k, z] = zero
        return carry

    lax.fori_loop(0, nz, clear, 0)

    sub = lax.broadcasted_iota(jnp.int32, (nx, ny), 0)
    lane = lax.broadcasted_iota(jnp.int32, (nx, ny), 1)
    w = [jnp.full((nx, ny), width_ref[k], jnp.int32).astype(jnp.float32) for k in range(4)]
    x_pos = (sub + row * nx).astype(jnp.float32)
    y_pos = (lane + col * ny).astype(jnp.float32)
    x_before = (jnp.zeros_like(sub) + (row * nx - 1)).astype(jnp.float32)
    y_before = (jnp.zeros_like(sub) + (col * ny - 1)).astype(jnp.float32)
    full_x, full_y = float(nx * n_row), float(ny * n_col)
    pairs = (
        absorber(x_pos + 0.5, full_x, w[0], w[1]), absorber(y_pos + 0.5, full_y, w[2], w[3]),
        absorber(x_pos, full_x, w[0], w[1]), absorber(y_pos, full_y, w[2], w[3]),
        absorber(x_before + 0.5, full_x, w[0], w[1]), absorber(y_before + 0.5, full_y, w[2], w[3]),
    )
    for k, (damp, gain) in enumerate(pairs):
        prof[2 * k] = damp
        prof[2 * k + 1] = gain

    def pack(z, ex, ey, ez, cols):
        first, last0, last1 = cols
        first_x[0, pl.ds(z, 1), :] = ey[0:1]
        first_x[1, pl.ds(z, 1), :] = ez[0:1]
        last_x[0, pl.ds(z, 1), :] = ex[nx - 1:nx]
        last_x[1, pl.ds(z, 1), :] = ey[nx - 1:nx]
        last_x[2, pl.ds(z, 1), :] = ez[nx - 1:nx]
        rx = pltpu.roll(ex, z, 1)
        rz = pltpu.roll(ez, z + nz, 1)
        ry = pltpu.roll(ey, z, 1)
        first = jnp.where(lane == z, rx, jnp.where(lane == z + nz, rz, first))
        before = lax.rem(z + ny - 1, ny)
        last0 = jnp.where(lane == before, rx, jnp.where(lane == z + nz - 1, rz, last0))
        last1 = jnp.where(lane == before, ry, last1)
        return first, last0, last1

    def keep(cols):
        first_y[1] = cols[0]
        last_y[0] = pltpu.roll(cols[1], 1, 1)
        last_y[1] = pltpu.roll(cols[2], 1, 1)

    def remote(m, src, dst, send, recv):
        return pltpu.make_async_remote_copy(
            src_ref=src, dst_ref=dst, send_sem=send, recv_sem=recv,
            device_id=routes[m][1], device_id_type=pl.DeviceIdType.MESH)

    def copy_of(m, slot, k=None):
        if m < 2:
            here = pl.ds(pl.multiple_of(k * UNROLL, UNROLL), UNROLL)
            src, dst = ((first_x, next_x), (last_x, prev_x))[m]
            return remote(
                m, src.at[:, here], dst.at[slot, :, here], x_send.at[m, slot, k], x_recv.at[m, slot, k])
        src, dst = {
            2: (first_y.at[1], next_y.at[slot, 1]), 3: (first_y.at[1], corner_x.at[slot]),
            4: (last_y, prev_y.at[slot]), 5: (last_y.at[1], corner_y.at[slot]),
            6: (first_y.at[0], next_y.at[slot, 0]),
        }[m]
        return remote(m, src, dst, send_sem.at[m, slot], recv_sem.at[m, slot])

    def start(m, slot, k=None):
        @pl.when(routes[m][0])
        def _():
            copy_of(m, slot, k).start()

    arrives = (down, up, right, ne, left, sw, right)

    def wait_recv(m, slot, k=None):
        @pl.when(arrives[m])
        def _():
            copy_of(m, slot, k).wait_recv()

    def wait_send(m, slot, k=None):
        @pl.when(routes[m][0])
        def _():
            copy_of(m, slot, k).wait_send()

    load_e.wait()
    load_h.wait()

    def first_pack(k, carry):
        cols, hcol = carry
        for j in range(UNROLL):
            z = k * UNROLL + j
            cols = pack(z, e_s[0, z], e_s[1, z], e_s[2, z], cols)
            hx, hy, hz = h_s[0, z + 1], h_s[1, z + 1], h_s[2, z + 1]
            h_last_x[0, pl.ds(z, 1), :] = hy[nx - 1:nx]
            h_last_x[1, pl.ds(z, 1), :] = hz[nx - 1:nx]
            hcol = jnp.where(lane == z, pltpu.roll(hz, z + 1, 1), hcol)
            hcol = jnp.where(lane == z + nz, pltpu.roll(hx, lax.rem(z + nz + 1, ny), 1), hcol)
        return cols, hcol

    cols, hcol = lax.fori_loop(0, nz // UNROLL, first_pack, ((zero, zero, zero), zero))
    keep(cols)
    first_y[0] = cols[0]
    h_last_y[...] = hcol

    count = n_row - 1 + n_col - 1 + sw.astype(jnp.int32) + ne.astype(jnp.int32)
    pl.semaphore_wait(barrier, count)
    once = [
        pltpu.make_async_remote_copy(
            src_ref=src, dst_ref=dst, send_sem=once_send.at[k], recv_sem=once_recv.at[k],
            device_id=routes[m][1], device_id_type=pl.DeviceIdType.MESH)
        for k, (src, dst, m) in enumerate(((h_last_x, halo_x, 1), (h_last_y, halo_y, 4)))
    ]
    for k in range(chunks):
        start(0, 0, k)
        start(1, 0, k)
    for m in (2, 4, 6, 3, 5):
        start(m, 0)
    for k, m in enumerate((1, 4)):
        @pl.when(routes[m][0])
        def _():
            once[k].start()
    load_c.wait()
    piece = n_modes // STEPS

    def mode_copies(s):
        return [
            pltpu.make_async_remote_copy(
                src_ref=basis_in.at[pl.ds(s * piece, piece), pl.ds(pl.multiple_of(peer * nx, nx), nx)],
                dst_ref=modes_3d.at[pl.ds(row * n_modes + s * piece, piece)],
                send_sem=mode_send.at[k, s], recv_sem=mode_recv.at[k, s],
                device_id={"row": peer, "col": col}, device_id_type=pl.DeviceIdType.MESH)
            for k, peer in enumerate(row_peers)
        ]

    def magnetic(slot):
        hdx, hgx, hdy, hgy = prof[0], prof[1], prof[2], prof[3]

        def body(k, carry):
            wait_recv(0, slot, k)

            @pl.when(k == 0)
            def _():
                wait_recv(6, slot)

            @pl.when(k == half)
            def _():
                wait_recv(2, slot)

            edge = next_y[slot, k // half]
            for j in range(UNROLL):
                z = k * UNROLL + j
                ex, ey, ez = e_s[0, z], e_s[1, z], e_s[2, z]
                row_y = jnp.broadcast_to(next_x[slot, 0, pl.ds(z, 1), :], (nx, ny))
                row_z = jnp.broadcast_to(next_x[slot, 1, pl.ds(z, 1), :], (nx, ny))
                col_x = pltpu.roll(edge, ny - 1 - z, 1)
                col_z = pltpu.roll(edge, ny - 1 - nz - z, 1)
                ey_dz = e_s[1, z + 1] - ey
                ex_dz = e_s[0, z + 1] - ex
                ez_dy = jnp.where(lane == ny - 1, col_z, pltpu.roll(ez, ny - 1, 1)) - ez
                ex_dy = jnp.where(lane == ny - 1, col_x, pltpu.roll(ex, ny - 1, 1)) - ex
                ez_dx = jnp.where(sub == nx - 1, row_z, pltpu.roll(ez, nx - 1, 0)) - ez
                ey_dx = jnp.where(sub == nx - 1, row_y, pltpu.roll(ey, nx - 1, 0)) - ey
                p0 = hdy * psi[0, z] + hgy * ez_dy
                p1 = hdx * psi[1, z] + hgx * ez_dx
                p2 = hdx * psi[2, z] + hgx * ey_dx
                p3 = hdy * psi[3, z] + hgy * ex_dy
                psi[0, z], psi[1, z], psi[2, z], psi[3, z] = p0, p1, p2, p3
                h_s[0, z + 1] = h_s[0, z + 1] - time_step * (ez_dy + p0 - ey_dz)
                h_s[1, z + 1] = h_s[1, z + 1] - time_step * (ex_dz - ez_dx - p1)
                h_s[2, z + 1] = h_s[2, z + 1] - time_step * (ey_dx + p2 - ex_dy - p3)
            return carry

        lax.fori_loop(0, nz // UNROLL, body, 0)

    def magnetic_row_before(slot):
        hdy, hgy = prof[2][0:1], prof[3][0:1]
        hdx, hgx = prof[8][0:1], prof[9][0:1]
        ex, ey, ez = prev_x[slot, 0, 0:nz], prev_x[slot, 1, 0:nz], prev_x[slot, 2, 0:nz]
        big_lane = lax.broadcasted_iota(jnp.int32, (nz, ny), 1)
        big_z = lax.broadcasted_iota(jnp.int32, (nz, ny), 0)
        corner = jnp.broadcast_to(corner_x[slot, nx - 1:nx, :], (nz, ny))
        corner = jnp.sum(jnp.where(big_lane == big_z, corner, 0.0), axis=1, keepdims=True)
        ex_dz = prev_x[slot, 0, 1:nz + 1] - ex
        ex_dy = jnp.where(big_lane == ny - 1, corner, pltpu.roll(ex, ny - 1, 1)) - ex
        ey_dx = first_x[0] - ey
        ez_dx = first_x[1] - ez
        p1 = hdx * halo_psi_x[0] + hgx * ez_dx
        p2 = hdx * halo_psi_x[1] + hgx * ey_dx
        p3 = hdy * halo_psi_x[2] + hgy * ex_dy
        halo_psi_x[0], halo_psi_x[1], halo_psi_x[2] = p1, p2, p3
        mask = up.astype(jnp.float32)
        halo_x[0] = mask * (halo_x[0] - time_step * (ex_dz - ez_dx - p1))
        halo_x[1] = mask * (halo_x[1] - time_step * (ey_dx + p2 - ex_dy - p3))

    def magnetic_column_before(slot):
        hdx, hgx = prof[0], prof[1]
        hdy, hgy = prof[10], prof[11]
        ey = prev_y[slot, 1]
        dy = first_y[1] - prev_y[slot, 0]
        below = jnp.broadcast_to(corner_y[slot, 0:1, :], (nx, ny))
        ey_dx = jnp.where(sub == nx - 1, below, pltpu.roll(ey, nx - 1, 0)) - ey
        ey_dz = pltpu.roll(pltpu.roll(ey, ny - 1, 1) - ey, nz, 1)
        py = hdy * halo_psi_y[0] + hgy * dy
        px = hdx * halo_psi_y[1] + hgx * ey_dx
        halo_psi_y[0], halo_psi_y[1] = py, px
        mask = left.astype(jnp.float32)
        change = jnp.where(lane < nz, ey_dx + px - dy - py, dy + py - ey_dz)
        halo_y[...] = mask * (halo_y[...] - time_step * change)

    def electric(s, slot):
        edx, egx, edy, egy = prof[4], prof[5], prof[6], prof[7]
        edge = halo_y[...]

        def body(k, cols):
            for j in range(UNROLL):
                z = k * UNROLL + j
                hx, hy, hz = h_s[0, z + 1], h_s[1, z + 1], h_s[2, z + 1]
                row_y = jnp.broadcast_to(halo_x[0, pl.ds(z, 1), :], (nx, ny))
                row_z = jnp.broadcast_to(halo_x[1, pl.ds(z, 1), :], (nx, ny))
                col_z = pltpu.roll(edge, lax.rem(ny - z, ny), 1)
                col_x = pltpu.roll(edge, ny - nz - z, 1)
                hy_dz = hy - h_s[1, z]
                hx_dz = hx - h_s[0, z]
                hz_dy = hz - jnp.where(lane == 0, col_z, pltpu.roll(hz, 1, 1))
                hx_dy = hx - jnp.where(lane == 0, col_x, pltpu.roll(hx, 1, 1))
                hz_dx = hz - jnp.where(sub == 0, row_z, pltpu.roll(hz, 1, 0))
                hy_dx = hy - jnp.where(sub == 0, row_y, pltpu.roll(hy, 1, 0))
                p0 = edy * psi[4, z] + egy * hz_dy
                p1 = edx * psi[5, z] + egx * hz_dx
                p2 = edx * psi[6, z] + egx * hy_dx
                p3 = edy * psi[7, z] + egy * hx_dy
                psi[4, z], psi[5, z], psi[6, z], psi[7, z] = p0, p1, p2, p3
                amount = coef_s[z]
                ex = e_s[0, z] + amount * (hz_dy + p0 - hy_dz)
                ey = e_s[1, z] + amount * (hx_dz - hz_dx - p1)
                ez = e_s[2, z] + amount * (hy_dx + p2 - hx_dy - p3)
                e_s[0, z], e_s[1, z], e_s[2, z] = ex, ey, ez
                cols = pack(z, ex, ey, ez, cols)
            more = s < STEPS - 1

            @pl.when(more)
            def _():
                start(0, slot, k)
                start(1, slot, k)

            @pl.when(k == half - 1)
            def _():
                first_y[0] = cols[0]

                @pl.when(more)
                def _():
                    start(6, slot)

            return cols

        keep(lax.fori_loop(0, nz // UNROLL, body, (zero, zero, zero)))

    def step(s, carry):
        slot = lax.rem(s, 2)
        for copy in mode_copies(s):
            copy.start()
        magnetic(slot)
        for k in range(chunks):
            wait_recv(1, slot, k)
        wait_recv(3, slot)

        @pl.when(s == 0)
        def _():
            for k, there in enumerate((up, left)):
                @pl.when(there)
                def _():
                    once[k].wait_recv()

        magnetic_row_before(slot)
        wait_recv(4, slot)
        wait_recv(5, slot)
        magnetic_column_before(slot)
        for k in range(chunks):
            wait_send(0, slot, k)
            wait_send(1, slot, k)
        for m in range(2, 7):
            wait_send(m, slot)
        electric(s, 1 - slot)

        @pl.when(s < STEPS - 1)
        def _():
            for m in (2, 4, 3, 5):
                start(m, 1 - slot)

        return carry

    lax.fori_loop(0, STEPS, step, 0)
    for k, m in enumerate((1, 4)):
        @pl.when(routes[m][0])
        def _():
            once[k].wait_send()
    store_e = pltpu.make_async_copy(e_s.at[:, pl.ds(0, nz)], e_out, local_sem.at[0])
    store_h = pltpu.make_async_copy(h_s.at[:, pl.ds(1, nz)], h_out, local_sem.at[1])
    store_e.start()
    store_h.start()

    count = snaps.shape[0] // nx

    def pick(s, carry):
        planes = []
        for j in range(8):
            index = index_ref[s * 8 + j]
            c = index // nz
            planes.append(fields[c, index - c * nz + (c // 3)])
        for j in range(8):
            snaps[pl.ds(pl.multiple_of((s * 8 + j) * nx, nx), nx), :] = planes[j]
        return carry

    lax.fori_loop(0, count // 8, pick, 0)
    load_b.wait()

    def wait_modes(s, carry):
        for copy in mode_copies(s):
            copy.wait()
        return carry

    lax.fori_loop(0, STEPS, wait_modes, 0)
    n_all = modes.shape[0] // nx
    dims = (((1,), (1,)), ((), ()))
    proj, gram = None, None
    for x in range(nx):
        a = snaps[pl.ds(x, count, stride=nx), :]
        b = modes[pl.ds(x, n_all, stride=nx), :]
        p = lax.dot_general(a, b, dims, precision=lax.Precision.HIGHEST, preferred_element_type=jnp.float32)
        g = lax.dot_general(a, a, dims, precision=lax.Precision.HIGHEST, preferred_element_type=jnp.float32)
        proj, gram = (p, g) if x == 0 else (proj + p, gram + g)
    part[:, 0:n_all] = proj
    part[:, n_all:n_all + count] = gram / float(nx * n_row * ny * n_col)

    share = count // n_row
    own = pl.ds(pl.multiple_of(row * share, share), share)

    def exchange(peers, axis, src_of, dst, sends, recvs):
        result = []
        for k, peer in enumerate(peers):
            where = {"row": row, "col": col}
            where[axis] = peer
            result.append(pltpu.make_async_remote_copy(
                src_ref=src_of(peer), dst_ref=dst, send_sem=sends.at[k], recv_sem=recvs.at[k],
                device_id=where, device_id_type=pl.DeviceIdType.MESH))
        for copy in result:
            copy.start()
        for copy in result:
            copy.wait()

    row_sums[row] = part[own, :]
    exchange(
        row_peers, "row", lambda peer: part.at[pl.ds(pl.multiple_of(peer * share, share), share)],
        row_sums.at[row], sum_send, sum_recv)
    value = row_sums[0]
    for k in range(1, n_row):
        value = value + row_sums[k]
    col_sums[col] = value
    exchange(col_peers, "col", lambda peer: col_sums.at[col], col_sums.at[col], col_send, col_recv)
    value = col_sums[0]
    for k in range(1, n_col):
        value = value + col_sums[k]
    total[own, :] = value
    exchange(row_peers, "row", lambda peer: total.at[own], total.at[own], back_send, back_recv)
    proj_out[...] = total[:, 0:n_all]
    gram_out[...] = total[:, n_all:n_all + count]
    store_e.wait()
    store_h.wait()


def shards(e_field, h_field, e_coef, basis, pml_width, snap_index):
    nz, nx, ny = e_coef.shape
    n_row, n_col = lax.axis_size("row"), lax.axis_size("col")
    modes, count = basis.shape[0] * n_row, snap_index.shape[0]
    f32 = jnp.float32
    wide = modes + (count + 127) // 128 * 128
    any_space = pl.BlockSpec(memory_space=pl.ANY)
    smem, vmem = pl.BlockSpec(memory_space=pltpu.SMEM), pl.BlockSpec(memory_space=pltpu.VMEM)
    return pl.pallas_call(
        functools.partial(step_kernel, n_row, n_col),
        out_shape=[
            jax.ShapeDtypeStruct(e_field.shape, f32), jax.ShapeDtypeStruct(h_field.shape, f32),
            jax.ShapeDtypeStruct((count, modes), f32), jax.ShapeDtypeStruct((count, count), f32),
        ],
        in_specs=[smem, smem, any_space, any_space, any_space, any_space],
        out_specs=[any_space, any_space, vmem, vmem],
        scratch_shapes=[
            pltpu.VMEM((6, nz + 1, nx, ny), f32),
            pltpu.VMEM((nz, nx, ny), f32), pltpu.VMEM((8, nz, nx, ny), f32),
            pltpu.VMEM((2, nz, ny), f32), pltpu.VMEM((3, nz, ny), f32), pltpu.VMEM((2, nz, ny), f32),
            pltpu.VMEM((2, nx, ny), f32), pltpu.VMEM((2, nx, ny), f32), pltpu.VMEM((nx, ny), f32),
            pltpu.VMEM((2, 2, nz, ny), f32), pltpu.VMEM((2, 3, nz + 8, ny), f32),
            pltpu.VMEM((2, nz, ny), f32), pltpu.VMEM((3, nz, ny), f32),
            pltpu.VMEM((2, 2, nx, ny), f32), pltpu.VMEM((2, 2, nx, ny), f32),
            pltpu.VMEM((2, nx, ny), f32), pltpu.VMEM((2, nx, ny), f32),
            pltpu.VMEM((nx, ny), f32), pltpu.VMEM((2, nx, ny), f32),
            pltpu.VMEM((12, nx, ny), f32),
            pltpu.VMEM((modes * nx, ny), f32), pltpu.VMEM((count * nx, ny), f32),
            pltpu.VMEM((count, wide), f32), pltpu.VMEM((n_row, count // n_row, wide), f32),
            pltpu.VMEM((n_col, count // n_row, wide), f32), pltpu.VMEM((count, wide), f32),
            pltpu.SemaphoreType.DMA((4,)),
            pltpu.SemaphoreType.DMA((2, 2, nz // UNROLL)), pltpu.SemaphoreType.DMA((2, 2, nz // UNROLL)),
            pltpu.SemaphoreType.DMA((7, 2)), pltpu.SemaphoreType.DMA((7, 2)),
            pltpu.SemaphoreType.DMA((2,)), pltpu.SemaphoreType.DMA((2,)),
            pltpu.SemaphoreType.DMA((n_row - 1, STEPS)), pltpu.SemaphoreType.DMA((n_row - 1, STEPS)),
            pltpu.SemaphoreType.DMA((n_row - 1,)), pltpu.SemaphoreType.DMA((n_row - 1,)),
            pltpu.SemaphoreType.DMA((n_col - 1,)), pltpu.SemaphoreType.DMA((n_col - 1,)),
            pltpu.SemaphoreType.DMA((n_row - 1,)), pltpu.SemaphoreType.DMA((n_row - 1,)),
        ],
        compiler_params=pltpu.CompilerParams(
            collective_id=0, has_side_effects=True, vmem_limit_bytes=67_043_328
        ),
    )(pml_width, snap_index, e_field, h_field, e_coef, basis)


def solution(mesh):
    in_specs = (
        P(None, None, "row", "col"),
        P(None, None, "row", "col"),
        P(None, "row", "col"),
        P("row", None, "col"),
        P(),
        P(),
    )
    out_specs = (P(None, None, "row", "col"), P(None, None, "row", "col"), P(), P())
    return jax.shard_map(shards, mesh=mesh, in_specs=in_specs, out_specs=out_specs, check_vma=False)
```
